128 devices in a mesh: row: 16 (over x, z), col: 8 (over y, core).
Axes of the slice: x: 4, y: 4, z: 4, core: 2. Of those that a mesh axis runs over, the one named last changes fastest.
Arguments:
- gradient: bfloat16 [3072, 14336], P('row', 'col'), may hold values from -0.1875 to 0.1875
- left_factor: float32 [3072, 3072], P('row', 'col'), may hold values from -1 to 11, as said below
- right_factor: float32 [14336, 14336], P('col', 'row'), may hold values from -1 to 3, as said below
- left_basis: bfloat16 [3072, 3072], P('row', 'col'), may hold values from -0.109375 to 0.109375
- right_basis: bfloat16 [14336, 2048], P('row', 'col'), may hold values from -0.046875 to 0.046875
Outputs:
- left_new: float32 [3072, 3072], P('row', 'col')
- right_new: float32 [14336, 14336], P('col', 'row')
- left_out: float32 [3072, 3072], P('row', 'col')
- right_out: float32 [14336, 2048], P('col', 'row')
The draws below stay inside these ranges and needn't reach their ends.
Inputs may be any that keep to these rules, and one draw needn't show every extreme that they name: left_factor is symmetric. right_factor is symmetric.
All inputs are finite; a program needn't handle non-finite values.
Results may differ from the reference program's by a relative error of at most 0.0029.
Values may be sent and summed in bfloat16 or wider, within the bound.
A program may use at most 128 MiB of HBM per device.

```python
import math
import jax
import jax.numpy as jnp
from jax import lax

DMODEL = 3072
DHIDDEN = 14336
NVEC = 2048


def factor_draw(key, size, level):
    noise = jax.random.truncated_normal(jax.random.fold_in(key, 11), -4.0, 4.0, (size, size), jnp.float32)
    noise = noise * (0.4 / math.sqrt(size))
    symmetric = noise + noise.T
    place = jnp.arange(size, dtype=jnp.float32) / size
    spread = jax.random.uniform(jax.random.fold_in(key, 12), (size,), jnp.float32, -1.2, 1.2)
    scaling = jnp.sqrt(level * jnp.exp(math.log(3.0) * place + spread))
    base = jnp.eye(size, dtype=jnp.float32) + symmetric
    return scaling[:, None] * base * scaling[None, :]


def draw_left_factor(key, part):
    return factor_draw(jax.random.fold_in(key, 21), DMODEL, 1.0)


def draw_right_factor(key, part):
    return factor_draw(jax.random.fold_in(key, 22), DHIDDEN, DMODEL / DHIDDEN)


def steps_of(own_key, shape, shards, least, top_value):
    loudness, own = 1.0, jax.random.fold_in(own_key, 6)
    for position, shards_of in shards:
        heights = jnp.exp(jax.random.uniform(jax.random.fold_in(own, position), (shards_of,), jnp.float32, least / len(shards), top_value / len(shards)))
        loudness = loudness * jnp.repeat(heights, shape[position] // shards_of).reshape([-1 if axis == position else 1 for axis in range(len(shape))])
    return loudness


def scatter_about(stream_key, extent, scale, limit, pieces=(), held_as=jnp.bfloat16):
    array = jax.random.normal(stream_key, extent, jnp.float32) * scale
    if len(pieces) > 0:
        array = steps_of(stream_key, extent, pieces, -0.22, 0.18) * array
    return jnp.clip(array, min=-limit, max=limit).astype(held_as)


def setup_inputs(seed: int = 0) -> dict:
    streams_of = jax.random.split(jax.random.key(seed), 6)
    return {
        "gradient": scatter_about(streams_of[0], (DMODEL, DHIDDEN), (DHIDDEN // 16) ** -0.5, 0.1875, ((0, 16), (1, 8))),
        "left_factor": draw_left_factor(jax.random.fold_in(streams_of[5], 71), 0),
        "right_factor": draw_right_factor(jax.random.fold_in(streams_of[5], 71), 0),
        "left_basis": scatter_about(streams_of[3], (DMODEL, DMODEL), DMODEL ** -0.5, 0.109375, ((0, 16), (1, 8))),
        "right_basis": scatter_about(streams_of[4], (DHIDDEN, NVEC), DHIDDEN ** -0.5, 0.046875, ((0, 16), (1, 8))),
    }


ema_decay = 0.95
epsilon = 1e-06

def reference(gradient, left_factor, right_factor, left_basis, right_basis):
    gram_left = lax.dot_general(gradient, gradient, (((1,), (1,)), ((), ())), preferred_element_type=jnp.float32)
    gram_right = lax.dot_general(gradient, gradient, (((0,), (0,)), ((), ())), preferred_element_type=jnp.float32)
    left_new = ema_decay * left_factor + (1.0 - ema_decay) * gram_left
    right_new = ema_decay * right_factor + (1.0 - ema_decay) * gram_right
    left_half = left_new.astype(jnp.bfloat16)
    right_half = right_new.astype(jnp.bfloat16)
    left_prod = jnp.dot(left_half, left_basis, preferred_element_type=jnp.float32)
    right_prod = jnp.dot(right_half, right_basis, preferred_element_type=jnp.float32)
    left_sq = lax.optimization_barrier(jnp.sum(left_prod * left_prod, axis=0))
    right_sq = lax.optimization_barrier(jnp.sum(right_prod * right_prod, axis=0))
    left_out = left_prod * lax.rsqrt(left_sq / DMODEL + epsilon)
    right_out = right_prod * lax.rsqrt(right_sq / DHIDDEN + epsilon)
    return (left_new, right_new, left_out, right_out)
```

```python
import functools

import jax
import jax.numpy as jnp
from jax import lax
from jax.experimental import pallas as pl
from jax.experimental.pallas import tpu as pltpu
from jax.sharding import PartitionSpec as P

DMODEL = 3072
DHIDDEN = 14336
ema_decay = 0.95
epsilon = 1e-06
MESH = pl.DeviceIdType.MESH
F32 = jnp.float32
BF16 = jnp.bfloat16
GC = 1792
LC = 384
W = GC + LC
SC = 896
FIRST, SECOND = "f", "s"


def wrap(v):
    return (v + 1) % 4 - 1


def message_table():
    keys = []
    for h in (0, 1):
        for axis in (FIRST, SECOND):
            for d in (1, -1):
                keys.append((h, 0, 0, "full", axis, d))
        keys.append((h, -1, 0, 0, FIRST, 1))
        keys.append((h, 1, 0, 1, FIRST, -1))
        for df in (-1, 1, 2):
            for d in (1, -1):
                keys.append((h, df, 0, "full", SECOND, d))
        for df in (0, -1, 1, 2):
            keys.append((h, df, -1, 0, SECOND, 1))
            keys.append((h, df, 1, 1, SECOND, -1))
    return {key: i for i, key in enumerate(keys)}


AG = message_table()
UNITS = [
    [(0, 0)],
    [(-1, 0), (1, 0)],
    [(0, -1), (0, 1)],
    [(2, 0)],
    [(-1, -1), (1, -1), (-1, 1), (1, 1)],
    [(0, 2)],
    [(2, -1), (2, 1)],
    [(-1, 2), (1, 2)],
    [(2, 2)],
]


def gather_kernel(
    grad, lbas, rbas, acc_o, bas_o, lb_o, lp_o,
    slab, shared, acc, bas, lp,
    ag_s, ag_r, y_s, y_r, sib_s, sib_r, loc, bs, br, bss, bsr, cp,
):
    row = lax.axis_index("row")
    col = lax.axis_index("col")
    x, z = row // 4, row % 4
    y, k = col // 2, col % 2
    sib = {"col": y * 2 + (1 - k)}

    def ydev(d):
        return {"col": ((y + d + 4) % 4) * 2 + k}

    def rid(dx, dz):
        return ((x + dx + 4) % 4) * 4 + (z + dz + 4) % 4

    def region(ref, h, df, ds, part):
        dx, dz = (df, ds) if h == 0 else (ds, df)
        q, n = (0, 2) if part == "full" else (part, 1)
        return ref.at[pl.ds(rid(dx, dz) * 4 + 2 * h + q, n)]

    def neighbour(h, axis, d):
        if (h == 0) == (axis == FIRST):
            return {"row": ((x + d + 4) % 4) * 4 + z}
        return {"row": x * 4 + (z + d + 4) % 4}

    def ag(h, df, ds, part, axis, d):
        i = AG[(h, df, ds, part, axis, d)]
        ref = region(slab, h, df, ds, part)
        return pltpu.make_async_remote_copy(
            src_ref=ref, dst_ref=ref, send_sem=ag_s.at[i], recv_sem=ag_r.at[i],
            device_id=neighbour(h, axis, d), device_id_type=MESH,
        )

    def ag_wait(h, df, ds, part, axis, d):
        key = (h, wrap(df + d), ds, part, axis, d) if axis == FIRST else (h, df, wrap(ds + d), part, axis, d)
        i = AG[key]
        ref = region(slab, h, df, ds, part)
        pltpu.make_async_remote_copy(
            src_ref=ref, dst_ref=ref, send_sem=ag_s.at[i], recv_sem=ag_r.at[i],
            device_id=neighbour(h, axis, d), device_id_type=MESH,
        ).wait_recv()

    own = [
        pltpu.make_async_copy(grad, slab.at[pl.ds(row * 4, 4), :, pl.ds(0, GC)], cp.at[0]),
        pltpu.make_async_copy(lbas, slab.at[pl.ds(row * 4, 4), :, pl.ds(GC, LC)], cp.at[1]),
        pltpu.make_async_copy(rbas, bas.at[col], cp.at[2]),
    ]
    for c in own:
        c.start()

    barrier = pltpu.get_barrier_semaphore()
    peers = [neighbour(0, a, d) for a in (FIRST, SECOND) for d in (1, -1)] + [ydev(1), ydev(-1), sib]
    for peer in peers:
        pl.semaphore_signal(barrier, inc=1, device_id=peer, device_id_type=MESH)
    for c in own:
        c.wait()
    pl.semaphore_wait(barrier, len(peers))

    is_k = k == z // 2
    role = (y - x + 4) % 4
    source = jnp.logical_and(is_k, role == 0)
    relay = jnp.logical_and(is_k, role != 0)
    c0 = pl.multiple_of((z % 2) * SC, 128)

    def unit_id(h, df, ds):
        return h * 16 + (df + 1) * 4 + ds + 1

    def unit_region(h, df, ds):
        return region(shared, h, df, ds, "full")

    def unit_src(h, df, ds):
        dx, dz = (df, ds) if h == 0 else (ds, df)
        return slab.at[pl.ds(rid(dx, dz) * 4 + 2 * h, 2), :, pl.ds(c0, SC)]

    def to_y(src, h, df, ds):
        i = unit_id(h, df, ds)
        return pltpu.make_async_remote_copy(
            src_ref=src, dst_ref=unit_region(h, df, ds), send_sem=y_s.at[i], recv_sem=y_r.at[i],
            device_id=ydev(1 if h == 0 else -1), device_id_type=MESH,
        )

    def to_sib(src, h, df, ds):
        i = unit_id(h, df, ds)
        return pltpu.make_async_remote_copy(
            src_ref=src, dst_ref=unit_region(h, df, ds), send_sem=sib_s.at[i], recv_sem=sib_r.at[i],
            device_id=sib, device_id_type=MESH,
        )

    def local(h, df, ds):
        return pltpu.make_async_copy(unit_src(h, df, ds), unit_region(h, df, ds), loc.at[unit_id(h, df, ds)])

    def last_role(h):
        return 3 if h == 0 else 1

    def source_units(step):
        @pl.when(source)
        def _():
            for df, ds in UNITS[step]:
                for h in (0, 1):
                    src = unit_src(h, df, ds)
                    to_y(src, h, df, ds).start()
                    to_sib(src, h, df, ds).start()
                    local(h, df, ds).start()

    def relay_units(step):
        @pl.when(relay)
        def _():
            for df, ds in UNITS[step]:
                for h in (0, 1):
                    ref = unit_region(h, df, ds)
                    to_y(ref, h, df, ds).wait_recv()

                    @pl.when(role != last_role(h))
                    def _():
                        to_y(ref, h, df, ds).start()

                    to_sib(ref, h, df, ds).start()

    def b_ref(dy, kk, part):
        c = ((y + dy + 4) % 4) * 2 + kk
        return bas.at[c] if part == "full" else bas.at[c, part]

    def b_send(i, dy, part, d):
        ref = b_ref(dy, k, part)
        return pltpu.make_async_remote_copy(
            src_ref=ref, dst_ref=ref, send_sem=bs.at[i], recv_sem=br.at[i], device_id=ydev(d), device_id_type=MESH,
        )

    def b_sib(i, dy, kk):
        ref = b_ref(dy, kk, "full")
        return pltpu.make_async_remote_copy(
            src_ref=ref, dst_ref=ref, send_sem=bss.at[i], recv_sem=bsr.at[i], device_id=sib, device_id_type=MESH,
        )

    def group(dx, first, last):
        xg = (x + dx + 4) % 4
        units = [(0, dx, dz) for dz in (-1, 0, 1, 2)] + [(1, dz, dx) for dz in (-1, 0, 1, 2)]

        @pl.when(jnp.logical_not(is_k))
        def _():
            for u in units:
                to_sib(unit_region(*u), *u).wait_recv()

        @pl.when(source)
        def _():
            for u in units:
                local(*u).wait()

        rows = pl.ds(xg * 16, 16)

        def tile(m, carry):
            cols = pl.ds(pl.multiple_of(m * 256, 256), 256)
            a = slab[rows, :, cols].reshape(768, 256)
            b = shared[rows].reshape(768, SC)
            d = lax.dot_general(a, b, (((0,), (0,)), ((), ())), preferred_element_type=F32)
            if first:
                acc[m] = d
            else:
                acc[m] = acc[m] + d
            if last:
                pltpu.make_async_copy(acc.at[m], acc_o.at[m], cp.at[m]).start()
            return carry

        lax.fori_loop(0, 7, tile, 0)

        def left(j, carry):
            a = slab[pl.ds(row * 4, 4), :, pl.ds(0, GC)].reshape(192, GC)
            b = slab[pl.ds(xg * 16 + j * 8, 8), :, pl.ds(0, GC)].reshape(384, GC)
            d = lax.dot_general(a, b, (((1,), (1,)), ((), ())), preferred_element_type=F32)
            lp[xg * 2 + j] = d.astype(BF16)
            return carry

        lax.fori_loop(0, 2, left, 0)

    sent = []

    def go(*key):
        c = ag(*key)
        c.start()
        sent.append(c)

    H = (0, 1)
    for axis in (FIRST, SECOND):
        for h in H:
            for d in (1, -1):
                go(h, 0, 0, "full", axis, d)
    b_sends = [b_send(0, 0, "full", 1), b_send(1, 0, "full", -1)]
    b_sibs = [b_sib(0, 0, k)]
    for c in b_sends + b_sibs:
        c.start()
    source_units(0)
    for h in H:
        ag_wait(h, -1, 0, "full", FIRST, 1)
        ag_wait(h, 1, 0, "full", FIRST, -1)
    for h in H:
        go(h, -1, 0, 0, FIRST, 1)
        go(h, 1, 0, 1, FIRST, -1)
    for df in (-1, 1):
        for h in H:
            for d in (1, -1):
                go(h, df, 0, "full", SECOND, d)
    source_units(1)
    relay_units(0)
    for h in H:
        ag_wait(h, 0, -1, "full", SECOND, 1)
        ag_wait(h, 0, 1, "full", SECOND, -1)
    for h in H:
        go(h, 0, -1, 0, SECOND, 1)
        go(h, 0, 1, 1, SECOND, -1)
    source_units(2)
    relay_units(1)
    b_send(0, -1, "full", 1).wait_recv()
    b_send(1, 1, "full", -1).wait_recv()
    more = [b_send(2, -1, 0, 1), b_send(3, 1, 1, -1)]
    more_sib = [b_sib(1, -1, k), b_sib(2, 1, k)]
    for c in more + more_sib:
        c.start()
    b_sends += more
    b_sibs += more_sib
    for h in H:
        ag_wait(h, 2, 0, 0, FIRST, 1)
        ag_wait(h, 2, 0, 1, FIRST, -1)
    for h in H:
        for d in (1, -1):
            go(h, 2, 0, "full", SECOND, d)
    source_units(3)
    relay_units(2)
    for df in (-1, 1):
        for h in H:
            ag_wait(h, df, -1, "full", SECOND, 1)
            ag_wait(h, df, 1, "full", SECOND, -1)
    for df in (-1, 1):
        for h in H:
            go(h, df, -1, 0, SECOND, 1)
            go(h, df, 1, 1, SECOND, -1)
    source_units(4)
    relay_units(3)
    b_send(2, 2, 0, 1).wait_recv()
    b_send(3, 2, 1, -1).wait_recv()
    c = b_sib(3, 2, k)
    c.start()
    b_sibs.append(c)
    for h in H:
        ag_wait(h, 0, 2, 0, SECOND, 1)
        ag_wait(h, 0, 2, 1, SECOND, -1)
    source_units(5)
    relay_units(4)
    for h in H:
        ag_wait(h, 2, -1, "full", SECOND, 1)
        ag_wait(h, 2, 1, "full", SECOND, -1)
    for h in H:
        go(h, 2, -1, 0, SECOND, 1)
        go(h, 2, 1, 1, SECOND, -1)
    source_units(6)
    relay_units(5)
    group(0, True, False)
    for df in (-1, 1):
        for h in H:
            ag_wait(h, df, 2, 0, SECOND, 1)
            ag_wait(h, df, 2, 1, SECOND, -1)
    source_units(7)
    relay_units(6)
    for h in H:
        ag_wait(h, 2, 2, 0, SECOND, 1)
        ag_wait(h, 2, 2, 1, SECOND, -1)
    source_units(8)
    lb_copy = pltpu.make_async_copy(slab.at[:, :, pl.ds(GC, LC)], lb_o, cp.at[7])
    lb_copy.start()
    relay_units(7)
    group(-1, False, False)
    relay_units(8)
    for i, dy in enumerate((0, -1, 1, 2)):
        b_sib(i, dy, 1 - k).wait_recv()
    bas_copy = pltpu.make_async_copy(bas, bas_o, cp.at[8])
    bas_copy.start()
    group(1, False, False)
    group(2, False, True)
    lp_copy = pltpu.make_async_copy(lp, lp_o, cp.at[9])
    lp_copy.start()

    for c in sent + b_sends + b_sibs:
        c.wait_send()
    for step in range(9):
        for df, ds in UNITS[step]:
            for h in H:
                ref = unit_region(h, df, ds)

                @pl.when(jnp.logical_and(is_k, jnp.logical_or(role == 0, role != last_role(h))))
                def _():
                    to_y(ref, h, df, ds).wait_send()

                @pl.when(is_k)
                def _():
                    to_sib(ref, h, df, ds).wait_send()

    for m in range(7):
        pltpu.make_async_copy(acc.at[m], acc_o.at[m], cp.at[m]).wait()
    lb_copy.wait()
    bas_copy.wait()
    lp_copy.wait()


def gather_all(gradient, left_basis, right_basis):
    dma = pltpu.SemaphoreType.DMA
    n = len(AG)
    any_spec = pl.BlockSpec(memory_space=pl.ANY)
    return pl.pallas_call(
        gather_kernel,
        out_shape=(
            jax.ShapeDtypeStruct((7, 256, SC), F32),
            jax.ShapeDtypeStruct((8, 2, 448, 256), BF16),
            jax.ShapeDtypeStruct((64, 48, LC), BF16),
            jax.ShapeDtypeStruct((8, 192, LC), BF16),
        ),
        in_specs=[any_spec] * 3,
        out_specs=[any_spec] * 4,
        scratch_shapes=[
            pltpu.VMEM((64, 48, W), BF16),
            pltpu.VMEM((64, 48, SC), BF16),
            pltpu.VMEM((7, 256, SC), F32),
            pltpu.VMEM((8, 2, 448, 256), BF16),
            pltpu.VMEM((8, 192, LC), BF16),
            dma((n,)), dma((n,)), dma((32,)), dma((32,)), dma((32,)), dma((32,)), dma((32,)),
            dma((4,)), dma((4,)), dma((4,)), dma((4,)), dma((10,)),
        ],
        compiler_params=pltpu.CompilerParams(
            collective_id=0, has_side_effects=True, vmem_limit_bytes=48 * 1024 * 1024
        ),
        name="gather_gram",
    )(gradient.reshape(4, 48, GC), left_basis.reshape(4, 48, LC), right_basis.reshape(2, 448, 256))


def product_kernel(acc, factor, basis, new, part):
    value = ema_decay * factor[...] + (1.0 - ema_decay) * acc[0]
    new[...] = value
    half = value.astype(BF16)
    for c in range(8):
        d = jnp.dot(half, basis[c], preferred_element_type=F32).astype(BF16)
        part[2 * c] = d[:, :128]
        part[2 * c + 1] = d[:, 128:]


def product(acc, factor, basis):
    return pl.pallas_call(
        product_kernel,
        grid=(7,),
        out_shape=(
            jax.ShapeDtypeStruct((GC, SC), F32),
            jax.ShapeDtypeStruct((16, GC, 128), BF16),
        ),
        in_specs=[
            pl.BlockSpec((1, 256, SC), lambda i: (i, 0, 0)),
            pl.BlockSpec((256, SC), lambda i: (i, 0)),
            pl.BlockSpec((8, SC, 256), lambda i: (0, 0, 0)),
        ],
        out_specs=(
            pl.BlockSpec((256, SC), lambda i: (i, 0)),
            pl.BlockSpec((16, 256, 128), lambda i: (0, i, 0)),
        ),
        compiler_params=pltpu.CompilerParams(vmem_limit_bytes=40 * 1024 * 1024),
        name="product",
    )(acc, factor, basis)


def on_device(gradient, left_factor, right_factor, left_basis, right_basis):
    acc, basis, lb, lp = gather_all(gradient, left_basis, right_basis)
    right_new, parts = product(acc, right_factor, basis.reshape(8, SC, 256))
    gram_block = jnp.sum(lax.all_to_all(lp, "col", 0, 0, tiled=True).astype(F32), axis=0)
    left_new = ema_decay * left_factor + (1.0 - ema_decay) * gram_block
    left_half = left_new.astype(BF16)
    left_rows = lax.all_gather(left_half, "col", axis=1, tiled=True)
    left_prod = jnp.dot(left_rows, lb.reshape(DMODEL, LC), preferred_element_type=F32)
    right_prod = jnp.sum(lax.all_to_all(parts, "row", 0, 0, tiled=True).astype(F32), axis=0)
    left_sq = lax.psum(jnp.sum(left_prod * left_prod, axis=0), "row")
    right_sq = lax.psum(jnp.sum(right_prod * right_prod, axis=0), "col")
    left_out = left_prod * lax.rsqrt(left_sq / DMODEL + epsilon)
    right_out = right_prod * lax.rsqrt(right_sq / DHIDDEN + epsilon)
    return (left_new, right_new, left_out, right_out)


def solution(mesh):
    in_specs = (P("row", "col"), P("row", "col"), P("col", "row"), P("row", "col"), P("row", "col"))
    out_specs = (P("row", "col"), P("col", "row"), P("row", "col"), P("col", "row"))
    return jax.shard_map(on_device, mesh=mesh, in_specs=in_specs, out_specs=out_specs, check_vma=False)
```

```python
import functools

import jax
import jax.numpy as jnp
from jax import lax
from jax.experimental import pallas as pl
from jax.experimental.pallas import tpu as pltpu
from jax.sharding import PartitionSpec as P

DMODEL = 3072
DHIDDEN = 14336
ema_decay = 0.95
epsilon = 1e-06
MESH = pl.DeviceIdType.MESH
F32 = jnp.float32
BF16 = jnp.bfloat16
GC = 1792
LC = 384
W = GC + LC
SC = 896
FIRST, SECOND = "f", "s"
TILES = ((0, 512), (512, 512), (1024, 512), (1536, 256))
PIECE = [n // 4 for _, n in TILES]
PLACE = [0, 128, 256, 384]
A1, B1, C1, A2, B2, C2 = range(6)


def wrap(v):
    return (v + 1) % 4 - 1


def message_table():
    keys = []
    for h in (0, 1):
        for axis in (FIRST, SECOND):
            for d in (1, -1):
                keys.append((h, 0, 0, "full", axis, d))
        keys.append((h, -1, 0, 0, FIRST, 1))
        keys.append((h, 1, 0, 1, FIRST, -1))
        for df in (-1, 1, 2):
            for d in (1, -1):
                keys.append((h, df, 0, "full", SECOND, d))
        for df in (0, -1, 1, 2):
            keys.append((h, df, -1, 0, SECOND, 1))
            keys.append((h, df, 1, 1, SECOND, -1))
    return {key: i for i, key in enumerate(keys)}


AG = message_table()
UNITS = [
    [(0, 0)],
    [(-1, 0), (1, 0)],
    [(0, -1), (0, 1)],
    [(2, 0)],
    [(-1, -1), (1, -1), (-1, 1), (1, 1)],
    [(0, 2)],
    [(2, -1), (2, 1)],
    [(-1, 2), (1, 2)],
    [(2, 2)],
]


def kernel(
    grad, lbas, rbas, rfac, lfac,
    rnew_o, rprod_o, rsum_o, lnew_o, lprod_o, lsum_o,
    slab, shared, acc, bas, lp, prod,
    ra, tb, rb, rc, s1, keep, ra2, tb2, rb2, rc2, rout, rsq,
    lrecv, lrows, lf, ln, lpr, lsq,
    ag_s, ag_r, y_s, y_r, sib_s, sib_r, loc, bs, br, bss, bsr, cp,
    rs_s, rs_r, l1s, l1r, l2s, l2r, l3s, l3r, q_s, q_r,
):
    row = lax.axis_index("row")
    col = lax.axis_index("col")
    x, z = row // 4, row % 4
    y, k = col // 2, col % 2
    sib = {"col": y * 2 + (1 - k)}

    def ydev(d):
        return {"col": ((y + d + 4) % 4) * 2 + k}

    def rid(dx, dz):
        return ((x + dx + 4) % 4) * 4 + (z + dz + 4) % 4

    def region(ref, h, df, ds, part):
        dx, dz = (df, ds) if h == 0 else (ds, df)
        q, n = (0, 2) if part == "full" else (part, 1)
        return ref.at[pl.ds(rid(dx, dz) * 4 + 2 * h + q, n)]

    def neighbour(h, axis, d):
        if (h == 0) == (axis == FIRST):
            return {"row": ((x + d + 4) % 4) * 4 + z}
        return {"row": x * 4 + (z + d + 4) % 4}

    def ag(h, df, ds, part, axis, d):
        i = AG[(h, df, ds, part, axis, d)]
        ref = region(slab, h, df, ds, part)
        return pltpu.make_async_remote_copy(
            src_ref=ref, dst_ref=ref, send_sem=ag_s.at[i], recv_sem=ag_r.at[i],
            device_id=neighbour(h, axis, d), device_id_type=MESH,
        )

    def ag_wait(h, df, ds, part, axis, d):
        key = (h, wrap(df + d), ds, part, axis, d) if axis == FIRST else (h, df, wrap(ds + d), part, axis, d)
        i = AG[key]
        ref = region(slab, h, df, ds, part)
        pltpu.make_async_remote_copy(
            src_ref=ref, dst_ref=ref, send_sem=ag_s.at[i], recv_sem=ag_r.at[i],
            device_id=neighbour(h, axis, d), device_id_type=MESH,
        ).wait_recv()

    own = [
        pltpu.make_async_copy(grad, slab.at[pl.ds(row * 4, 4), :, pl.ds(0, GC)], cp.at[0]),
        pltpu.make_async_copy(lbas, slab.at[pl.ds(row * 4, 4), :, pl.ds(GC, LC)], cp.at[1]),
        pltpu.make_async_copy(rbas, bas.at[col], cp.at[2]),
    ]
    late = [
        pltpu.make_async_copy(rfac, acc, cp.at[3]),
        pltpu.make_async_copy(lfac, lf, cp.at[4]),
    ]
    for c in own + late:
        c.start()

    def colmate(i):
        return {"col": (col + i) % 8}

    def rowmate(i):
        return {"row": (row + i) % 16}

    barrier = pltpu.get_barrier_semaphore()

    def greet(make, n):
        def body(i, carry):
            pl.semaphore_signal(barrier, inc=1, device_id=make(i), device_id_type=MESH)
            return carry

        lax.fori_loop(1, n, body, 0)

    greet(colmate, 8)
    greet(rowmate, 16)
    for c in own:
        c.wait()
    pl.semaphore_wait(barrier, 22)

    is_k = k == z // 2
    role = (y - x + 4) % 4
    source = jnp.logical_and(is_k, role == 0)
    relay = jnp.logical_and(is_k, role != 0)
    c0 = pl.multiple_of((z % 2) * SC, 128)

    def unit_id(h, df, ds):
        return h * 16 + (df + 1) * 4 + ds + 1

    def unit_region(h, df, ds):
        return region(shared, h, df, ds, "full")

    def unit_src(h, df, ds):
        dx, dz = (df, ds) if h == 0 else (ds, df)
        return slab.at[pl.ds(rid(dx, dz) * 4 + 2 * h, 2), :, pl.ds(c0, SC)]

    def to_y(src, h, df, ds):
        i = unit_id(h, df, ds)
        return pltpu.make_async_remote_copy(
            src_ref=src, dst_ref=unit_region(h, df, ds), send_sem=y_s.at[i], recv_sem=y_r.at[i],
            device_id=ydev(1 if h == 0 else -1), device_id_type=MESH,
        )

    def to_sib(src, h, df, ds):
        i = unit_id(h, df, ds)
        return pltpu.make_async_remote_copy(
            src_ref=src, dst_ref=unit_region(h, df, ds), send_sem=sib_s.at[i], recv_sem=sib_r.at[i],
            device_id=sib, device_id_type=MESH,
        )

    def local(h, df, ds):
        return pltpu.make_async_copy(unit_src(h, df, ds), unit_region(h, df, ds), loc.at[unit_id(h, df, ds)])

    def last_role(h):
        return 3 if h == 0 else 1

    def source_units(step):
        @pl.when(source)
        def _():
            for df, ds in UNITS[step]:
                for h in (0, 1):
                    src = unit_src(h, df, ds)
                    to_y(src, h, df, ds).start()
                    to_sib(src, h, df, ds).start()
                    local(h, df, ds).start()

    def hop(h):
        return role if h == 0 else (4 - role) % 4

    def relay_units(step):
        for hops, lag in ((1, 1), (2, 1), (3, 2)):
            if not 0 <= step - lag <= 8:
                continue
            for h in (0, 1):

                @pl.when(jnp.logical_and(is_k, hop(h) == hops))
                def _():
                    for df, ds in UNITS[step - lag]:
                        ref = unit_region(h, df, ds)
                        to_y(ref, h, df, ds).wait_recv()
                        if hops < 3:
                            to_y(ref, h, df, ds).start()
                        to_sib(ref, h, df, ds).start()

    def b_ref(dy, kk, part):
        c = ((y + dy + 4) % 4) * 2 + kk
        return bas.at[c] if part == "full" else bas.at[c, part]

    def b_send(i, dy, part, d):
        ref = b_ref(dy, k, part)
        return pltpu.make_async_remote_copy(
            src_ref=ref, dst_ref=ref, send_sem=bs.at[i], recv_sem=br.at[i], device_id=ydev(d), device_id_type=MESH,
        )

    def b_sib(i, dy, kk):
        ref = b_ref(dy, kk, "full")
        return pltpu.make_async_remote_copy(
            src_ref=ref, dst_ref=ref, send_sem=bss.at[i], recv_sem=bsr.at[i], device_id=sib, device_id_type=MESH,
        )

    def group_ready(dx):
        units = [(0, dx, dz) for dz in (-1, 0, 1, 2)] + [(1, dz, dx) for dz in (-1, 0, 1, 2)]

        @pl.when(jnp.logical_not(is_k))
        def _():
            for u in units:
                to_sib(unit_region(*u), *u).wait_recv()

        @pl.when(source)
        def _():
            for u in units:
                local(*u).wait()

    def gram(dx, first, lo, hi):
        xg = (x + dx + 4) % 4
        rows = pl.ds(xg * 16, 16)

        def tile(m, carry):
            cols = pl.ds(pl.multiple_of(m * 256, 256), 256)
            a = slab[rows, :, cols].reshape(768, 256)
            b = shared[rows].reshape(768, SC)
            d = lax.dot_general(a, b, (((0,), (0,)), ((), ())), preferred_element_type=F32)
            old = acc[cols, :]
            if first:
                old = ema_decay * old
            acc[cols, :] = old + (1.0 - ema_decay) * d
            return carry

        lax.fori_loop(lo, hi, tile, 0)

    def l1(c, mine):
        return pltpu.make_async_remote_copy(
            src_ref=lp.at[c], dst_ref=lrecv.at[mine], send_sem=l1s.at[c], recv_sem=l1r.at[mine],
            device_id={"col": c}, device_id_type=MESH,
        )

    def left(dx):
        xg = (x + dx + 4) % 4

        def part(j, carry):
            c = xg * 2 + j
            a = slab[pl.ds(row * 4, 4), :, pl.ds(0, GC)].reshape(192, GC)
            b = slab[pl.ds(xg * 16 + j * 8, 8), :, pl.ds(0, GC)].reshape(384, GC)
            d = lax.dot_general(a, b, (((1,), (1,)), ((), ())), preferred_element_type=F32)
            lp[c] = d.astype(BF16)

            @pl.when(c != col)
            def _():
                l1(c, col).start()

            return carry

        lax.fori_loop(0, 2, part, 0)

    def l2(i):
        return pltpu.make_async_remote_copy(
            src_ref=lrows.at[col], dst_ref=lrows.at[col], send_sem=l2s.at[i], recv_sem=l2r.at[i],
            device_id=colmate(i), device_id_type=MESH,
        )

    def l3(i):
        return pltpu.make_async_remote_copy(
            src_ref=lsq.at[row], dst_ref=lsq.at[row], send_sem=l3s.at[i], recv_sem=l3r.at[i],
            device_id=rowmate(i), device_id_type=MESH,
        )

    def rq(i):
        return pltpu.make_async_remote_copy(
            src_ref=rsq.at[col], dst_ref=rsq.at[col], send_sem=q_s.at[i], recv_sem=q_r.at[i],
            device_id=colmate(i), device_id_type=MESH,
        )

    def each(n, make, what):
        def body(i, carry):
            c = make(i)
            getattr(c, what)()
            return carry

        lax.fori_loop(1, n, body, 0)

    def left_refresh():
        total = lp[col].astype(F32)
        for i in range(1, 8):
            c = (col + i) % 8
            l1(c, c).wait_recv()
            total = total + lrecv[c].astype(F32)
        new = ema_decay * lf[...] + (1.0 - ema_decay) * total
        ln[...] = new
        lrows[col] = new.astype(BF16)
        each(8, l2, "start")
        pltpu.make_async_copy(ln, lnew_o, cp.at[5]).start()

    def left_product():
        each(8, l2, "wait_recv")

        def part(c, carry):
            b = slab[pl.ds(c * 8, 8), :, pl.ds(GC, LC)].reshape(384, LC)
            return carry + jnp.dot(lrows[c], b, preferred_element_type=F32)

        lpr[...] = lax.fori_loop(0, 8, part, jnp.zeros((192, LC), F32))
        v = lpr[...]
        lsq[row] = jnp.broadcast_to(jnp.sum(v * v, axis=0, keepdims=True), (8, LC))
        each(16, l3, "start")
        pltpu.make_async_copy(lpr, lprod_o, cp.at[6]).start()

    def make_product(t):
        lo, n = TILES[t]
        pltpu.make_async_copy(acc.at[pl.ds(lo, n)], rnew_o.at[pl.ds(lo, n)], cp.at[8 + t]).start()

        def part(i, carry):
            c, r = i // 2, i % 2
            start = pl.multiple_of(lo + r * (n // 2), 128)
            half = acc[pl.ds(start, n // 2), :].astype(BF16)
            d = jnp.dot(half, bas[c].reshape(SC, 256), preferred_element_type=F32).astype(BF16)
            xo, zo = c // 2, (c % 2) * 2
            prod[xo, zo, pl.ds(start, n // 2), :] = d[:, :128]
            prod[xo, zo + 1, pl.ds(start, n // 2), :] = d[:, 128:]
            return carry

        lax.fori_loop(0, 16, part, 0)

    TYPES = (0, 1, 2, 3)

    def hd(i):
        return i // 2, 1 if i % 2 == 0 else -1

    def rows_of(i, t):
        return pl.ds(TILES[t][0] + i * PIECE[t], PIECE[t])

    def spot(t):
        return pl.ds(PLACE[t], PIECE[t])

    def pos(h, axis):
        return x if (h == 0) == (axis == FIRST) else z

    def chunk(i, t, e):
        h, _ = hd(i)
        p = (pos(h, FIRST) + e + 4) % 4
        return prod.at[p, :, rows_of(i, t), :] if h == 0 else prod.at[:, p, rows_of(i, t), :]

    def rs(kind, i, t):
        h, d = hd(i)
        axis = FIRST if kind < A2 else SECOND
        q = (pos(h, SECOND) + 4) % 4
        if kind == A1:
            src, dst, to = chunk(i, t, 2), ra.at[i, :, spot(t), :], d
        elif kind == B1:
            src, dst, to = tb.at[i, :, spot(t), :], rb.at[i, :, spot(t), :], d
        elif kind == C1:
            src, dst, to = chunk(i, t, -d), rc.at[i, :, spot(t), :], -d
        elif kind == A2:
            src, dst, to = s1.at[i, (q + 2) % 4, spot(t), :], ra2.at[i, spot(t), :], d
        elif kind == B2:
            src, dst, to = tb2.at[i, spot(t), :], rb2.at[i, spot(t), :], d
        else:
            src, dst, to = s1.at[i, (q - d + 4) % 4, spot(t), :], rc2.at[i, spot(t), :], -d
        return pltpu.make_async_remote_copy(
            src_ref=src, dst_ref=dst, send_sem=rs_s.at[kind, i * 4 + t], recv_sem=rs_r.at[kind, i * 4 + t],
            device_id=neighbour(h, axis, to), device_id_type=MESH,
        )

    def r0(t):
        for kind in (A1, C1):
            for i in TYPES:
                rs(kind, i, t).start()

    def r1(t):
        for i in TYPES:
            h, d = hd(i)
            rs(A1, i, t).wait_recv()
            mine = chunk(i, t, d)
            tb[i, :, spot(t), :] = (mine[...].astype(F32) + ra[i, :, spot(t), :].astype(F32)).astype(BF16)
            rs(B1, i, t).start()

    def r2(t):
        for i in TYPES:
            h, d = hd(i)
            rs(C1, i, t).wait_recv()
            rs(B1, i, t).wait_recv()
            mine = chunk(i, t, 0)
            q = pos(h, SECOND)

            s1[i, :, spot(t), :] = (
                mine[...].astype(F32) + rb[i, :, spot(t), :].astype(F32) + rc[i, :, spot(t), :].astype(F32)
            ).astype(BF16)
            rs(A2, i, t).start()
            rs(C2, i, t).start()
            own_chunk = prod.at[x, z, rows_of(i, t), :]
            keep[i, spot(t), :] = (
                own_chunk[...].astype(F32) + rb[i, q, spot(t), :].astype(F32) + rc[i, q, spot(t), :].astype(F32)
            )

    def r3(t):
        for i in TYPES:
            h, d = hd(i)
            q = (pos(h, SECOND) + d + 4) % 4
            rs(A2, i, t).wait_recv()
            tb2[i, spot(t), :] = (s1[i, q, spot(t), :].astype(F32) + ra2[i, spot(t), :].astype(F32)).astype(BF16)
            rs(B2, i, t).start()

    def r4(t):
        total = jnp.zeros((8, 128), F32)
        for i in TYPES:
            rs(C2, i, t).wait_recv()
            rs(B2, i, t).wait_recv()
            v = keep[i, spot(t), :] + rb2[i, spot(t), :].astype(F32) + rc2[i, spot(t), :].astype(F32)
            rout[rows_of(i, t), :] = v
            total = total + jnp.sum((v * v).reshape(PIECE[t] // 8, 8, 128), axis=0)
        lo, n = TILES[t]
        pltpu.make_async_copy(rout.at[pl.ds(lo, n)], rprod_o.at[pl.ds(lo, n)], cp.at[12 + t]).start()
        return total

    sent = []

    def go(*key):
        c = ag(*key)
        c.start()
        sent.append(c)

    H = (0, 1)
    for axis in (FIRST, SECOND):
        for h in H:
            for d in (1, -1):
                go(h, 0, 0, "full", axis, d)
    b_sends = [b_send(0, 0, "full", 1), b_send(1, 0, "full", -1)]
    b_sibs = [b_sib(0, 0, k)]
    for c in b_sends + b_sibs:
        c.start()
    source_units(0)
    for h in H:
        ag_wait(h, -1, 0, "full", FIRST, 1)
        ag_wait(h, 1, 0, "full", FIRST, -1)
    for h in H:
        go(h, -1, 0, 0, FIRST, 1)
        go(h, 1, 0, 1, FIRST, -1)
    for df in (-1, 1):
        for h in H:
            for d in (1, -1):
                go(h, df, 0, "full", SECOND, d)
    source_units(1)
    relay_units(1)
    for h in H:
        ag_wait(h, 0, -1, "full", SECOND, 1)
        ag_wait(h, 0, 1, "full", SECOND, -1)
    for h in H:
        go(h, 0, -1, 0, SECOND, 1)
        go(h, 0, 1, 1, SECOND, -1)
    source_units(2)
    relay_units(2)
    b_send(0, -1, "full", 1).wait_recv()
    b_send(1, 1, "full", -1).wait_recv()
    more = [b_send(2, -1, 0, 1), b_send(3, 1, 1, -1)]
    more_sib = [b_sib(1, -1, k), b_sib(2, 1, k)]
    for c in more + more_sib:
        c.start()
    b_sends += more
    b_sibs += more_sib
    for h in H:
        ag_wait(h, 2, 0, 0, FIRST, 1)
        ag_wait(h, 2, 0, 1, FIRST, -1)
    for h in H:
        for d in (1, -1):
            go(h, 2, 0, "full", SECOND, d)
    source_units(3)
    relay_units(3)
    for df in (-1, 1):
        for h in H:
            ag_wait(h, df, -1, "full", SECOND, 1)
            ag_wait(h, df, 1, "full", SECOND, -1)
    for df in (-1, 1):
        for h in H:
            go(h, df, -1, 0, SECOND, 1)
            go(h, df, 1, 1, SECOND, -1)
    source_units(4)
    relay_units(4)
    b_send(2, 2, 0, 1).wait_recv()
    b_send(3, 2, 1, -1).wait_recv()
    c = b_sib(3, 2, k)
    c.start()
    b_sibs.append(c)
    for h in H:
        ag_wait(h, 0, 2, 0, SECOND, 1)
        ag_wait(h, 0, 2, 1, SECOND, -1)
    source_units(5)
    relay_units(5)
    for h in H:
        ag_wait(h, 2, -1, "full", SECOND, 1)
        ag_wait(h, 2, 1, "full", SECOND, -1)
    for h in H:
        go(h, 2, -1, 0, SECOND, 1)
        go(h, 2, 1, 1, SECOND, -1)
    source_units(6)
    relay_units(6)
    for df in (-1, 1):
        for h in H:
            ag_wait(h, df, 2, 0, SECOND, 1)
            ag_wait(h, df, 2, 1, SECOND, -1)
    source_units(7)
    relay_units(7)
    late[0].wait()
    group_ready(0)
    gram(0, True, 0, 7)
    left(0)
    for h in H:
        ag_wait(h, 2, 2, 0, SECOND, 1)
        ag_wait(h, 2, 2, 1, SECOND, -1)
    source_units(8)
    relay_units(8)
    relay_units(9)
    group_ready(-1)
    gram(-1, False, 0, 7)
    left(-1)
    relay_units(10)
    group_ready(1)
    gram(1, False, 0, 7)
    left(1)
    for i, dy in enumerate((0, -1, 1, 2)):
        b_sib(i, dy, 1 - k).wait_recv()
    group_ready(2)
    gram(2, False, 0, 2)
    make_product(0)
    r0(0)
    gram(2, False, 2, 4)
    make_product(1)
    r0(1)
    r1(0)
    gram(2, False, 4, 6)
    make_product(2)
    r0(2)
    r1(1)
    gram(2, False, 6, 7)
    make_product(3)
    r0(3)
    left(2)
    r1(2)
    r2(0)
    late[1].wait()
    r1(3)
    r3(0)
    r2(1)
    left_refresh()
    total = r4(0)
    r3(1)
    r2(2)
    total = total + r4(1)
    r3(2)
    left_product()
    r2(3)
    total = total + r4(2)
    r3(3)
    total = total + r4(3)
    rsq[col] = total
    each(8, rq, "start")

    each(16, l3, "wait_recv")
    lsum = pltpu.make_async_copy(lsq, lsum_o, cp.at[7])
    lsum.start()
    each(8, rq, "wait_recv")
    rsum = pltpu.make_async_copy(rsq, rsum_o, cp.at[16])
    rsum.start()

    for c in sent + b_sends + b_sibs:
        c.wait_send()
    for step in range(9):
        for df, ds in UNITS[step]:
            for h in H:
                ref = unit_region(h, df, ds)

                @pl.when(jnp.logical_and(is_k, hop(h) != 3))
                def _():
                    to_y(ref, h, df, ds).wait_send()

                @pl.when(is_k)
                def _():
                    to_sib(ref, h, df, ds).wait_send()

    for kind in range(6):
        for i in TYPES:
            for t in range(4):
                rs(kind, i, t).wait_send()
    for i in range(1, 8):
        l1((col + i) % 8, col).wait_send()
    each(8, l2, "wait_send")
    each(16, l3, "wait_send")
    each(8, rq, "wait_send")
    for t, (lo, n) in enumerate(TILES):
        pltpu.make_async_copy(acc.at[pl.ds(lo, n)], rnew_o.at[pl.ds(lo, n)], cp.at[8 + t]).wait()
        pltpu.make_async_copy(rout.at[pl.ds(lo, n)], rprod_o.at[pl.ds(lo, n)], cp.at[12 + t]).wait()
    pltpu.make_async_copy(ln, lnew_o, cp.at[5]).wait()
    pltpu.make_async_copy(lpr, lprod_o, cp.at[6]).wait()
    lsum.wait()
    rsum.wait()


def refresh(gradient, left_basis, right_basis, right_factor, left_factor):
    dma = pltpu.SemaphoreType.DMA
    n = len(AG)
    any_spec = pl.BlockSpec(memory_space=pl.ANY)
    V = pltpu.VMEM
    return pl.pallas_call(
        kernel,
        out_shape=(
            jax.ShapeDtypeStruct((GC, SC), F32),
            jax.ShapeDtypeStruct((GC, 128), F32),
            jax.ShapeDtypeStruct((8, 8, 128), F32),
            jax.ShapeDtypeStruct((192, LC), F32),
            jax.ShapeDtypeStruct((192, LC), F32),
            jax.ShapeDtypeStruct((16, 8, LC), F32),
        ),
        in_specs=[any_spec] * 5,
        out_specs=[any_spec] * 6,
        scratch_shapes=[
            V((64, 48, W), BF16), V((64, 48, SC), BF16), V((GC, SC), F32), V((8, 2, 448, 256), BF16),
            V((8, 192, LC), BF16), V((4, 4, GC, 128), BF16),
            V((4, 4, 448, 128), BF16), V((4, 4, 448, 128), BF16), V((4, 4, 448, 128), BF16),
            V((4, 4, 448, 128), BF16), V((4, 4, 448, 128), BF16), V((4, 448, 128), F32),
            V((4, 448, 128), BF16), V((4, 448, 128), BF16), V((4, 448, 128), BF16), V((4, 448, 128), BF16),
            V((GC, 128), F32), V((8, 8, 128), F32),
            V((8, 192, LC), BF16), V((8, 192, LC), BF16), V((192, LC), F32), V((192, LC), F32), V((192, LC), F32),
            V((16, 8, LC), F32),
            dma((n,)), dma((n,)), dma((32,)), dma((32,)), dma((32,)), dma((32,)), dma((32,)),
            dma((4,)), dma((4,)), dma((4,)), dma((4,)), dma((17,)),
            dma((6, 16)), dma((6, 16)), dma((8,)), dma((8,)), dma((8,)), dma((8,)), dma((16,)), dma((16,)),
            dma((8,)), dma((8,)),
        ],
        compiler_params=pltpu.CompilerParams(
            collective_id=0, has_side_effects=True, vmem_limit_bytes=67043328
        ),
        name="refresh",
    )(
        gradient.reshape(4, 48, GC), left_basis.reshape(4, 48, LC), right_basis.reshape(2, 448, 256),
        right_factor, left_factor,
    )


def on_device(gradient, left_factor, right_factor, left_basis, right_basis):
    right_new, right_prod, rsq, left_new, left_prod, lsq = refresh(
        gradient, left_basis, right_basis, right_factor, left_factor
    )
    left_sq = jnp.sum(lsq[:, 0], axis=0)
    right_sq = jnp.sum(rsq, axis=(0, 1))
    left_out = left_prod * lax.rsqrt(left_sq / DMODEL + epsilon)
    right_out = right_prod * lax.rsqrt(right_sq / DHIDDEN + epsilon)
    return (left_new, right_new, left_out, right_out)


def solution(mesh):
    in_specs = (P("row", "col"), P("row", "col"), P("col", "row"), P("row", "col"), P("row", "col"))
    out_specs = (P("row", "col"), P("col", "row"), P("row", "col"), P("col", "row"))
    return jax.shard_map(on_device, mesh=mesh, in_specs=in_specs, out_specs=out_specs, check_vma=False)
```

```python
import functools

import jax
import jax.numpy as jnp
from jax import lax
from jax.experimental import pallas as pl
from jax.experimental.pallas import tpu as pltpu
from jax.sharding import PartitionSpec as P

DMODEL = 3072
DHIDDEN = 14336
ema_decay = 0.95
epsilon = 1e-06
MESH = pl.DeviceIdType.MESH
F32 = jnp.float32
BF16 = jnp.bfloat16
GC = 1792
LC = 384
SC = 896
FIRST, SECOND = "f", "s"
TILES = ((0, 512), (512, 512), (1024, 512), (1536, 256))
PIECE = [n // 4 for _, n in TILES]
PLACE = [0, 128, 256, 384]
A1, B1, C1, A2, B2, C2 = range(6)


def wrap(v):
    return (v + 1) % 4 - 1


def message_table():
    keys = []
    for h in (0, 1):
        for axis in (FIRST, SECOND):
            for d in (1, -1):
                keys.append((h, 0, 0, "full", axis, d))
        keys.append((h, -1, 0, 0, FIRST, 1))
        keys.append((h, 1, 0, 1, FIRST, -1))
        for df in (-1, 1, 2):
            for d in (1, -1):
                keys.append((h, df, 0, "full", SECOND, d))
        for df in (0, -1, 1, 2):
            keys.append((h, df, -1, 0, SECOND, 1))
            keys.append((h, df, 1, 1, SECOND, -1))
    return {key: i for i, key in enumerate(keys)}


AG = message_table()
UNITS = [
    (0, 0), (-1, 0), (1, 0), (0, -1), (0, 1), (2, 0), (-1, -1), (-1, 1), (1, -1), (1, 1),
    (0, 2), (2, -1), (2, 1), (-1, 2), (1, 2), (2, 2),
]
LAGS = (1, 2, 4)


def kernel(
    grad, lbas, rbas, rfac, lfac,
    rnew_o, rprod_o, rsum_o, lnew_o, lprod_o, lsum_o,
    slab, lbuf, shared, acc, bas, lp, away, near, both, whole,
    ra, tb, rb, rc, s1, keep, ra2, tb2, rb2, rc2, rout, rsq,
    lsib, lmid, lrecv, lrows, lf, ln, lpr, lsq,
    ag_s, ag_r, lg_s, lg_r, y_s, y_r, sib_s, sib_r, loc, bs, br, bss, bsr, cp,
    rs_s, rs_r, l0s, l0r, l1s, l1r, l2s, l2r, l4s, l4r, l3s, l3r, q_s, q_r,
):
    row = lax.axis_index("row")
    col = lax.axis_index("col")
    x, z = row // 4, row % 4
    y, k = col // 2, col % 2
    sib = {"col": y * 2 + (1 - k)}

    def ydev(d):
        return {"col": ((y + d + 4) % 4) * 2 + k}

    def rid(dx, dz):
        return ((x + dx + 4) % 4) * 4 + (z + dz + 4) % 4

    def region(ref, h, df, ds, part):
        dx, dz = (df, ds) if h == 0 else (ds, df)
        q, n = (0, 2) if part == "full" else (part, 1)
        return ref.at[pl.ds(rid(dx, dz) * 4 + 2 * h + q, n)]

    def neighbour(h, axis, d):
        if (h == 0) == (axis == FIRST):
            return {"row": ((x + d + 4) % 4) * 4 + z}
        return {"row": x * 4 + (z + d + 4) % 4}

    def ag(buf, ss, rr, h, df, ds, part, axis, d, arriving=False):
        if not arriving:
            key = (h, df, ds, part, axis, d)
        elif axis == FIRST:
            key = (h, wrap(df + d), ds, part, axis, d)
        else:
            key = (h, df, wrap(ds + d), part, axis, d)
        i = AG[key]
        ref = region(buf, h, df, ds, part)
        return pltpu.make_async_remote_copy(
            src_ref=ref, dst_ref=ref, send_sem=ss.at[i], recv_sem=rr.at[i],
            device_id=neighbour(h, axis, d), device_id_type=MESH,
        )

    def arrive(net, u):
        df, ds = UNITS[u]
        if u == 0:
            return
        axis = FIRST if ds == 0 else SECOND
        e = df if ds == 0 else ds
        for h in (0, 1):
            if e == 2:
                ag(*net, h, df, ds, 0, axis, 1, True).wait_recv()
                ag(*net, h, df, ds, 1, axis, -1, True).wait_recv()
            else:
                ag(*net, h, df, ds, "full", axis, -e, True).wait_recv()

    def onward(net, u):
        df, ds = UNITS[u]
        out = []
        if u == 0:
            for axis in (FIRST, SECOND):
                for h in (0, 1):
                    for d in (1, -1):
                        out.append((h, 0, 0, "full", axis, d))
        elif ds == 0:
            for h in (0, 1):
                if df == -1:
                    out.append((h, df, 0, 0, FIRST, 1))
                if df == 1:
                    out.append((h, df, 0, 1, FIRST, -1))
            for h in (0, 1):
                for d in (1, -1):
                    out.append((h, df, 0, "full", SECOND, d))
        elif ds != 2:
            for h in (0, 1):
                out.append((h, df, ds, 0 if ds == -1 else 1, SECOND, -ds))
        for key in out:
            c = ag(*net, *key)
            c.start()
            sent.append(c)

    sent = []
    G = (slab, ag_s, ag_r)
    L = (lbuf, lg_s, lg_r)

    own = [
        pltpu.make_async_copy(grad, slab.at[pl.ds(row * 4, 4)], cp.at[0]),
        pltpu.make_async_copy(lbas, lbuf.at[pl.ds(row * 4, 4)], cp.at[1]),
        pltpu.make_async_copy(rbas, bas.at[col], cp.at[2]),
    ]
    late = [
        pltpu.make_async_copy(rfac, acc, cp.at[3]),
        pltpu.make_async_copy(lfac, lf, cp.at[4]),
    ]
    for c in own + late:
        c.start()

    def colmate(i):
        return {"col": (col + i) % 8}

    def rowmate(i):
        return {"row": (row + i) % 16}

    barrier = pltpu.get_barrier_semaphore()

    def greet(make, n):
        def body(i, carry):
            pl.semaphore_signal(barrier, inc=1, device_id=make(i), device_id_type=MESH)
            return carry

        lax.fori_loop(1, n, body, 0)

    greet(colmate, 8)
    greet(rowmate, 16)
    for c in own:
        c.wait()
    pl.semaphore_wait(barrier, 22)

    is_k = k == z // 2
    role = (y - x + 4) % 4
    source = jnp.logical_and(is_k, role == 0)
    relay = jnp.logical_and(is_k, role != 0)
    c0 = pl.multiple_of((z % 2) * SC, 128)

    def unit_id(h, df, ds):
        return h * 16 + (df + 1) * 4 + ds + 1

    def unit_region(h, df, ds):
        return region(shared, h, df, ds, "full")

    def unit_src(h, df, ds):
        dx, dz = (df, ds) if h == 0 else (ds, df)
        return slab.at[pl.ds(rid(dx, dz) * 4 + 2 * h, 2), :, pl.ds(c0, SC)]

    def to_y(src, h, df, ds):
        i = unit_id(h, df, ds)
        return pltpu.make_async_remote_copy(
            src_ref=src, dst_ref=unit_region(h, df, ds), send_sem=y_s.at[i], recv_sem=y_r.at[i],
            device_id=ydev(1 if h == 0 else -1), device_id_type=MESH,
        )

    def to_sib(src, h, df, ds):
        i = unit_id(h, df, ds)
        return pltpu.make_async_remote_copy(
            src_ref=src, dst_ref=unit_region(h, df, ds), send_sem=sib_s.at[i], recv_sem=sib_r.at[i],
            device_id=sib, device_id_type=MESH,
        )

    def local(h, df, ds):
        return pltpu.make_async_copy(unit_src(h, df, ds), unit_region(h, df, ds), loc.at[unit_id(h, df, ds)])

    def last_role(h):
        return 3 if h == 0 else 1

    def source_unit(u):
        @pl.when(source)
        def _():
            df, ds = UNITS[u]
            for h in (0, 1):
                src = unit_src(h, df, ds)
                to_y(src, h, df, ds).start()
                to_sib(src, h, df, ds).start()
                local(h, df, ds).start()

    def hop(h):
        return role if h == 0 else (4 - role) % 4

    def relay_unit(hops, u):
        df, ds = UNITS[u]
        for h in (0, 1):

            @pl.when(jnp.logical_and(is_k, hop(h) == hops))
            def _():
                ref = unit_region(h, df, ds)
                to_y(ref, h, df, ds).wait_recv()
                if hops < 3:
                    to_y(ref, h, df, ds).start()
                to_sib(ref, h, df, ds).start()

    relayed = [0, 0, 0]

    def relay_to(hops, n):
        while relayed[hops - 1] < n:
            relay_unit(hops, relayed[hops - 1])
            relayed[hops - 1] += 1

    def b_ref(dy, kk, part):
        c = ((y + dy + 4) % 4) * 2 + kk
        return bas.at[c] if part == "full" else bas.at[c, part]

    def b_send(i, dy, part, d):
        ref = b_ref(dy, k, part)
        return pltpu.make_async_remote_copy(
            src_ref=ref, dst_ref=ref, send_sem=bs.at[i], recv_sem=br.at[i], device_id=ydev(d), device_id_type=MESH,
        )

    def b_sib(i, dy, kk):
        ref = b_ref(dy, kk, "full")
        return pltpu.make_async_remote_copy(
            src_ref=ref, dst_ref=ref, send_sem=bss.at[i], recv_sem=bsr.at[i], device_id=sib, device_id_type=MESH,
        )

    def group_ready(dx):
        units = [(0, dx, dz) for dz in (-1, 0, 1, 2)] + [(1, dz, dx) for dz in (-1, 0, 1, 2)]

        @pl.when(jnp.logical_not(is_k))
        def _():
            for u in units:
                to_sib(unit_region(*u), *u).wait_recv()

        @pl.when(source)
        def _():
            for u in units:
                local(*u).wait()

    def gram(dx, first, lo, hi):
        xg = (x + dx + 4) % 4
        rows = pl.ds(xg * 16, 16)

        def tile(m, carry):
            cols = pl.ds(pl.multiple_of(m * 256, 256), 256)
            a = slab[rows, :, cols].reshape(768, 256)
            b = shared[rows].reshape(768, SC)
            d = lax.dot_general(a, b, (((0,), (0,)), ((), ())), preferred_element_type=F32)
            old = acc[cols, :]
            if first:
                old = ema_decay * old
            acc[cols, :] = old + (1.0 - ema_decay) * d
            return carry

        lax.fori_loop(lo, hi, tile, 0)

    def l0(yy, c):
        return pltpu.make_async_remote_copy(
            src_ref=lp.at[c], dst_ref=lsib.at[yy], send_sem=l0s.at[yy], recv_sem=l0r.at[yy],
            device_id=sib, device_id_type=MESH,
        )

    def left(dx):
        xg = (x + dx + 4) % 4

        def part(j, carry):
            c = xg * 2 + j
            a = slab[pl.ds(row * 4, 4)].reshape(192, GC)
            b = slab[pl.ds(xg * 16 + j * 8, 8)].reshape(384, GC)
            d = lax.dot_general(a, b, (((1,), (1,)), ((), ())), preferred_element_type=F32)
            lp[c] = d.astype(BF16)

            @pl.when(j != k)
            def _():
                l0(xg, c).start()

            return carry

        lax.fori_loop(0, 2, part, 0)

    def l1(dy):
        yy = (y + dy) % 4
        return pltpu.make_async_remote_copy(
            src_ref=lmid.at[yy], dst_ref=lrecv.at[y], send_sem=l1s.at[dy], recv_sem=l1r.at[dy],
            device_id={"col": yy * 2 + k}, device_id_type=MESH,
        )

    def l2(dy):
        return pltpu.make_async_remote_copy(
            src_ref=lrows.at[col], dst_ref=lrows.at[col], send_sem=l2s.at[dy], recv_sem=l2r.at[dy],
            device_id={"col": ((y + dy) % 4) * 2 + k}, device_id_type=MESH,
        )

    def l4(yy, kk):
        c = yy * 2 + kk
        return pltpu.make_async_remote_copy(
            src_ref=lrows.at[c], dst_ref=lrows.at[c], send_sem=l4s.at[yy], recv_sem=l4r.at[yy],
            device_id=sib, device_id_type=MESH,
        )

    def l3(i):
        return pltpu.make_async_remote_copy(
            src_ref=lsq.at[row], dst_ref=lsq.at[row], send_sem=l3s.at[i], recv_sem=l3r.at[i],
            device_id=rowmate(i), device_id_type=MESH,
        )

    def rq(i):
        return pltpu.make_async_remote_copy(
            src_ref=rsq.at[col], dst_ref=rsq.at[col], send_sem=q_s.at[i], recv_sem=q_r.at[i],
            device_id=colmate(i), device_id_type=MESH,
        )

    def each(n, make, what):
        def body(i, carry):
            c = make(i)
            getattr(c, what)()
            return carry

        lax.fori_loop(1, n, body, 0)

    def left_join():
        for dy in (1, 3, 2):
            yy = (y + dy) % 4
            l0(yy, yy * 2 + k).wait_recv()
            lmid[yy] = (lp[yy * 2 + k].astype(F32) + lsib[yy].astype(F32)).astype(BF16)
            l1(dy).start()

    def left_refresh():
        l0(y, col).wait_recv()
        total = lp[col].astype(F32) + lsib[y].astype(F32)
        for dy in (1, 3, 2):
            l1(dy).wait_recv()
            total = total + lrecv[(y + 4 - dy) % 4].astype(F32)
        new = ema_decay * lf[...] + (1.0 - ema_decay) * total
        ln[...] = new
        lrows[col] = new.astype(BF16)
        for dy in (1, 3, 2):
            l2(dy).start()
        l4(y, k).start()
        pltpu.make_async_copy(ln, lnew_o, cp.at[5]).start()

    def left_share():
        for dy in (1, 3, 2):
            l2(dy).wait_recv()
            l4((y + 4 - dy) % 4, k).start()

    def left_product():
        for yy in range(4):
            l4(yy, 1 - k).wait_recv()

        def part(c, carry):
            b = lbuf[pl.ds(c * 8, 8)].reshape(384, LC)
            return carry + jnp.dot(lrows[c], b, preferred_element_type=F32)

        lpr[...] = lax.fori_loop(0, 8, part, jnp.zeros((192, LC), F32))
        v = lpr[...]
        lsq[row] = jnp.broadcast_to(jnp.sum(v * v, axis=0, keepdims=True), (8, LC))
        each(16, l3, "start")
        pltpu.make_async_copy(lpr, lprod_o, cp.at[6]).start()

    def make_product(t):
        lo, n = TILES[t]
        pltpu.make_async_copy(acc.at[pl.ds(lo, n)], rnew_o.at[pl.ds(lo, n)], cp.at[8 + t]).start()

        m = PIECE[t]

        def first(cc, carry):
            half = acc[pl.ds(lo, n // 2), :].astype(BF16)
            for e in range(4):
                c = ((x + e) % 4) * 2 + cc
                d = jnp.dot(half, bas[c].reshape(SC, 256), preferred_element_type=F32)
                for i in (0, 1):
                    for s in (0, 1):
                        v = d[i * m : (i + 1) * m, s * 128 : (s + 1) * 128]
                        if e == 2:
                            away[i, 0, cc * 2 + s, spot(t), :] = v.astype(BF16)
                        elif e == (3 if i == 0 else 1):
                            away[i, 1, cc * 2 + s, spot(t), :] = v.astype(BF16)
                        else:
                            near[i, 0 if e == 0 else 1, cc * 2 + s, spot(t), :] = v
            return carry

        lax.fori_loop(0, 2, first, 0)

        def second(c, carry):
            half = acc[pl.ds(lo + n // 2, n // 2), :].astype(BF16)
            d = jnp.dot(half, bas[c].reshape(SC, 256), preferred_element_type=F32)
            for i in (0, 1):
                for s in (0, 1):
                    v = d[i * m : (i + 1) * m, s * 128 : (s + 1) * 128]
                    both[i, (c % 2) * 2 + s, c // 2, spot(t), :] = v.astype(BF16)
                    whole[i, (c % 2) * 2 + s, c // 2, spot(t), :] = v
            return carry

        lax.fori_loop(0, 8, second, 0)

    TYPES = (0, 1, 2, 3)

    def hd(i):
        return i // 2, 1 if i % 2 == 0 else -1

    def rows_of(i, t):
        return pl.ds(TILES[t][0] + i * PIECE[t], PIECE[t])

    def spot(t):
        return pl.ds(PLACE[t], PIECE[t])

    def pos(h, axis):
        return x if (h == 0) == (axis == FIRST) else z

    def parcel(i, t, kind):
        h, d = hd(i)
        if h == 0:
            return away.at[i, 0 if kind == A1 else 1, :, spot(t), :]
        return both.at[i - 2, (z + (2 if kind == A1 else -d) + 4) % 4, :, spot(t), :]

    def kept(i, t, ahead):
        h, d = hd(i)
        if h == 0:
            return near.at[i, 1 if ahead else 0, :, spot(t), :]
        return whole.at[i - 2, (z + (d if ahead else 0) + 4) % 4, :, spot(t), :]

    def rs(kind, i, t):
        h, d = hd(i)
        axis = FIRST if kind < A2 else SECOND
        q = (pos(h, SECOND) + 4) % 4
        if kind == A1:
            src, dst, to = parcel(i, t, A1), ra.at[i, :, spot(t), :], d
        elif kind == B1:
            src, dst, to = tb.at[i, :, spot(t), :], rb.at[i, :, spot(t), :], d
        elif kind == C1:
            src, dst, to = parcel(i, t, C1), rc.at[i, :, spot(t), :], -d
        elif kind == A2:
            src, dst, to = s1.at[i, (q + 2) % 4, spot(t), :], ra2.at[i, spot(t), :], d
        elif kind == B2:
            src, dst, to = tb2.at[i, spot(t), :], rb2.at[i, spot(t), :], d
        else:
            src, dst, to = s1.at[i, (q - d + 4) % 4, spot(t), :], rc2.at[i, spot(t), :], -d
        return pltpu.make_async_remote_copy(
            src_ref=src, dst_ref=dst, send_sem=rs_s.at[kind, i * 4 + t], recv_sem=rs_r.at[kind, i * 4 + t],
            device_id=neighbour(h, axis, to), device_id_type=MESH,
        )

    def r0(t):
        for kind in (A1, C1):
            for i in TYPES:
                rs(kind, i, t).start()

    def r1(t):
        for i in TYPES:
            h, d = hd(i)
            rs(A1, i, t).wait_recv()
            tb[i, :, spot(t), :] = (kept(i, t, True)[...] + ra[i, :, spot(t), :].astype(F32)).astype(BF16)
            rs(B1, i, t).start()

    def r2(t):
        for i in TYPES:
            h, d = hd(i)
            rs(C1, i, t).wait_recv()
            rs(B1, i, t).wait_recv()
            total = kept(i, t, False)[...] + rb[i, :, spot(t), :].astype(F32) + rc[i, :, spot(t), :].astype(F32)
            s1[i, :, spot(t), :] = total.astype(BF16)
            rs(A2, i, t).start()
            rs(C2, i, t).start()
            q = pos(h, SECOND)
            for f, e in ((0, 0), (1, d)):
                w = (q + e + 4) % 4
                mine = kept(i, t, False).at[w]
                keep[f, i, spot(t), :] = (
                    mine[...] + rb[i, w, spot(t), :].astype(F32) + rc[i, w, spot(t), :].astype(F32)
                )

    def r3(t):
        for i in TYPES:
            h, d = hd(i)
            rs(A2, i, t).wait_recv()
            tb2[i, spot(t), :] = (keep[1, i, spot(t), :] + ra2[i, spot(t), :].astype(F32)).astype(BF16)
            rs(B2, i, t).start()

    def r4(t):
        total = jnp.zeros((8, 128), F32)
        for i in TYPES:
            rs(C2, i, t).wait_recv()
            rs(B2, i, t).wait_recv()
            v = keep[0, i, spot(t), :] + rb2[i, spot(t), :].astype(F32) + rc2[i, spot(t), :].astype(F32)
            rout[rows_of(i, t), :] = v
            total = total + jnp.sum((v * v).reshape(PIECE[t] // 8, 8, 128), axis=0)
        lo, n = TILES[t]
        pltpu.make_async_copy(rout.at[pl.ds(lo, n)], rprod_o.at[pl.ds(lo, n)], cp.at[12 + t]).start()
        return total

    H = (0, 1)
    b_sends, b_sibs = [], []

    def begin(send, sibs):
        for c in send + sibs:
            c.start()
        b_sends.extend(send)
        b_sibs.extend(sibs)

    for u in range(16):
        arrive(G, u)
        onward(G, u)
        source_unit(u)
        for hops in (1, 2, 3):
            relay_to(hops, u + 1 - LAGS[hops - 1])
        if u == 2:
            begin([b_send(0, 0, "full", 1), b_send(1, 0, "full", -1)], [b_sib(0, 0, k)])
        if u == 8:
            b_send(0, -1, "full", 1).wait_recv()
            b_send(1, 1, "full", -1).wait_recv()
            begin([b_send(2, -1, 0, 1), b_send(3, 1, 1, -1)], [b_sib(1, -1, k), b_sib(2, 1, k)])
        if u == 12:
            onward(L, 0)
    relay_to(1, 16)
    relay_to(2, 16)
    b_send(2, 2, 0, 1).wait_recv()
    b_send(3, 2, 1, -1).wait_recv()
    begin([], [b_sib(3, 2, k)])

    def lb(a, b):
        for u in range(a, b):
            arrive(L, u)
            onward(L, u)

    lb(1, 3)
    late[0].wait()
    relay_to(3, 11)
    group_ready(0)
    gram(0, True, 0, 7)
    lb(3, 6)
    relay_to(3, 14)
    group_ready(-1)
    gram(-1, False, 0, 7)
    lb(6, 10)
    relay_to(3, 15)
    group_ready(1)
    gram(1, False, 0, 7)
    lb(10, 13)
    relay_to(3, 16)
    for i, dy in enumerate((0, -1, 1, 2)):
        b_sib(i, dy, 1 - k).wait_recv()
    group_ready(2)
    gram(2, False, 0, 2)
    make_product(0)
    r0(0)
    gram(2, False, 2, 4)
    make_product(1)
    r0(1)
    for dx in (0, -1, 1, 2):
        left(dx)
    r1(0)
    gram(2, False, 4, 6)
    make_product(2)
    r0(2)
    left_join()
    r1(1)
    gram(2, False, 6, 7)
    make_product(3)
    r0(3)
    r1(2)
    lb(13, 16)
    r2(0)
    late[1].wait()
    left_refresh()
    r1(3)
    r3(0)
    r2(1)
    total = r4(0)
    left_share()
    r3(1)
    r2(2)
    total = total + r4(1)
    left_product()
    r3(2)
    r2(3)
    total = total + r4(2)
    r3(3)
    total = total + r4(3)
    rsq[col] = total
    each(8, rq, "start")

    each(16, l3, "wait_recv")
    lsum = pltpu.make_async_copy(lsq, lsum_o, cp.at[7])
    lsum.start()
    each(8, rq, "wait_recv")
    rsum = pltpu.make_async_copy(rsq, rsum_o, cp.at[16])
    rsum.start()

    for c in sent + b_sends + b_sibs:
        c.wait_send()
    for df, ds in UNITS:
        for h in H:
            ref = unit_region(h, df, ds)

            @pl.when(jnp.logical_and(is_k, hop(h) != 3))
            def _():
                to_y(ref, h, df, ds).wait_send()

            @pl.when(is_k)
            def _():
                to_sib(ref, h, df, ds).wait_send()

    for kind in range(6):
        for i in TYPES:
            for t in range(4):
                rs(kind, i, t).wait_send()
    for yy in range(4):
        l0(yy, yy * 2 + 1 - k).wait_send()
        l4(yy, k).wait_send()
    for dy in (1, 2, 3):
        l1(dy).wait_send()
        l2(dy).wait_send()
    each(16, l3, "wait_send")
    each(8, rq, "wait_send")
    for t, (lo, n) in enumerate(TILES):
        pltpu.make_async_copy(acc.at[pl.ds(lo, n)], rnew_o.at[pl.ds(lo, n)], cp.at[8 + t]).wait()
        pltpu.make_async_copy(rout.at[pl.ds(lo, n)], rprod_o.at[pl.ds(lo, n)], cp.at[12 + t]).wait()
    pltpu.make_async_copy(ln, lnew_o, cp.at[5]).wait()
    pltpu.make_async_copy(lpr, lprod_o, cp.at[6]).wait()
    lsum.wait()
    rsum.wait()


def refresh(gradient, left_basis, right_basis, right_factor, left_factor):
    dma = pltpu.SemaphoreType.DMA
    n = len(AG)
    any_spec = pl.BlockSpec(memory_space=pl.ANY)
    V = pltpu.VMEM
    return pl.pallas_call(
        kernel,
        out_shape=(
            jax.ShapeDtypeStruct((GC, SC), F32),
            jax.ShapeDtypeStruct((GC, 128), F32),
            jax.ShapeDtypeStruct((8, 8, 128), F32),
            jax.ShapeDtypeStruct((192, LC), F32),
            jax.ShapeDtypeStruct((192, LC), F32),
            jax.ShapeDtypeStruct((16, 8, LC), F32),
        ),
        in_specs=[any_spec] * 5,
        out_specs=[any_spec] * 6,
        scratch_shapes=[
            V((64, 48, GC), BF16), V((64, 48, LC), BF16), V((64, 48, SC), BF16), V((GC, SC), F32),
            V((8, 2, 448, 256), BF16), V((8, 192, LC), BF16),
            V((2, 2, 4, 448, 128), BF16), V((2, 2, 4, 448, 128), F32),
            V((2, 4, 4, 448, 128), BF16), V((2, 4, 4, 448, 128), F32),
            V((4, 4, 448, 128), BF16), V((4, 4, 448, 128), BF16), V((4, 4, 448, 128), BF16),
            V((4, 4, 448, 128), BF16), V((4, 4, 448, 128), BF16), V((2, 4, 448, 128), F32),
            V((4, 448, 128), BF16), V((4, 448, 128), BF16), V((4, 448, 128), BF16), V((4, 448, 128), BF16),
            V((GC, 128), F32), V((8, 8, 128), F32),
            V((4, 192, LC), BF16), V((4, 192, LC), BF16), V((4, 192, LC), BF16), V((8, 192, LC), BF16),
            V((192, LC), F32), V((192, LC), F32), V((192, LC), F32), V((16, 8, LC), F32),
            dma((n,)), dma((n,)), dma((n,)), dma((n,)),
            dma((32,)), dma((32,)), dma((32,)), dma((32,)), dma((32,)),
            dma((4,)), dma((4,)), dma((4,)), dma((4,)), dma((17,)),
            dma((6, 16)), dma((6, 16)),
            dma((4,)), dma((4,)), dma((4,)), dma((4,)), dma((4,)), dma((4,)), dma((4,)), dma((4,)),
            dma((16,)), dma((16,)), dma((8,)), dma((8,)),
        ],
        compiler_params=pltpu.CompilerParams(
            collective_id=0, has_side_effects=True, vmem_limit_bytes=67043328
        ),
        name="refresh",
    )(
        gradient.reshape(4, 48, GC), left_basis.reshape(4, 48, LC), right_basis.reshape(2, 448, 256),
        right_factor, left_factor,
    )


def on_device(gradient, left_factor, right_factor, left_basis, right_basis):
    right_new, right_prod, rsq, left_new, left_prod, lsq = refresh(
        gradient, left_basis, right_basis, right_factor, left_factor
    )
    left_sq = jnp.sum(lsq[:, 0], axis=0)
    right_sq = jnp.sum(rsq, axis=(0, 1))
    left_out = left_prod * lax.rsqrt(left_sq / DMODEL + epsilon)
    right_out = right_prod * lax.rsqrt(right_sq / DHIDDEN + epsilon)
    return (left_new, right_new, left_out, right_out)


def solution(mesh):
    in_specs = (P("row", "col"), P("row", "col"), P("col", "row"), P("row", "col"), P("row", "col"))
    out_specs = (P("row", "col"), P("col", "row"), P("row", "col"), P("col", "row"))
    return jax.shard_map(on_device, mesh=mesh, in_specs=in_specs, out_specs=out_specs, check_vma=False)
```

```python
import functools

import jax
import jax.numpy as jnp
from jax import lax
from jax.experimental import pallas as pl
from jax.experimental.pallas import tpu as pltpu
from jax.sharding import PartitionSpec as P

DMODEL = 3072
DHIDDEN = 14336
ema_decay = 0.95
epsilon = 1e-06
MESH = pl.DeviceIdType.MESH
F32 = jnp.float32
BF16 = jnp.bfloat16
GC = 1792
LC = 384
SC = 896
FIRST, SECOND = "f", "s"
TILES = ((0, 512), (512, 512), (1024, 512), (1536, 256))
PIECE = [n // 4 for _, n in TILES]
PLACE = [sum(PIECE[:t]) for t in range(len(TILES))]
A1, B1, C1, A2, B2, C2 = range(6)


def wrap(v):
    return (v + 1) % 4 - 1


def message_table():
    keys = []
    for h in (0, 1):
        for axis in (FIRST, SECOND):
            for d in (1, -1):
                keys.append((h, 0, 0, "full", axis, d))
        keys.append((h, -1, 0, 0, FIRST, 1))
        keys.append((h, 1, 0, 1, FIRST, -1))
        for df in (-1, 1, 2):
            for d in (1, -1):
                keys.append((h, df, 0, "full", SECOND, d))
        for df in (0, -1, 1, 2):
            keys.append((h, df, -1, 0, SECOND, 1))
            keys.append((h, df, 1, 1, SECOND, -1))
    return {key: i for i, key in enumerate(keys)}


AG = message_table()
UNITS = [
    (0, 0), (-1, 0), (1, 0), (0, -1), (0, 1), (2, 0), (-1, -1), (-1, 1), (1, -1), (1, 1),
    (0, 2), (2, -1), (2, 1), (-1, 2), (1, 2), (2, 2),
]
LAGS = (1, 2, 4)


def kernel(
    grad, lbas, rbas, rfac, lfac,
    rnew_o, rprod_o, rsum_o, lnew_o, lprod_o, lsum_o,
    slab, lbuf, shared, acc, bas, lp, away, near, both, whole,
    ra, tb, rb, rc, s1, keep, ra2, tb2, rb2, rc2, rout, rsq,
    lsib, lmid, lrecv, lrows, lf, ln, lpr, lsq,
    ag_s, ag_r, lg_s, lg_r, y_s, y_r, sib_s, sib_r, loc, bs, br, bss, bsr, cp,
    rs_s, rs_r, l0s, l0r, l1s, l1r, l2s, l2r, l4s, l4r, l3s, l3r, q_s, q_r,
):
    row = lax.axis_index("row")
    col = lax.axis_index("col")
    x, z = row // 4, row % 4
    y, k = col // 2, col % 2
    sib = {"col": y * 2 + (1 - k)}

    def ydev(d):
        return {"col": ((y + d + 4) % 4) * 2 + k}

    def rid(dx, dz):
        return ((x + dx + 4) % 4) * 4 + (z + dz + 4) % 4

    def region(ref, h, df, ds, part):
        dx, dz = (df, ds) if h == 0 else (ds, df)
        q, n = (0, 2) if part == "full" else (part, 1)
        return ref.at[pl.ds(rid(dx, dz) * 4 + 2 * h + q, n)]

    def neighbour(h, axis, d):
        if (h == 0) == (axis == FIRST):
            return {"row": ((x + d + 4) % 4) * 4 + z}
        return {"row": x * 4 + (z + d + 4) % 4}

    def ag(buf, ss, rr, h, df, ds, part, axis, d, arriving=False):
        if not arriving:
            key = (h, df, ds, part, axis, d)
        elif axis == FIRST:
            key = (h, wrap(df + d), ds, part, axis, d)
        else:
            key = (h, df, wrap(ds + d), part, axis, d)
        i = AG[key]
        ref = region(buf, h, df, ds, part)
        return pltpu.make_async_remote_copy(
            src_ref=ref, dst_ref=ref, send_sem=ss.at[i], recv_sem=rr.at[i],
            device_id=neighbour(h, axis, d), device_id_type=MESH,
        )

    def arrive(net, u):
        df, ds = UNITS[u]
        if u == 0:
            return
        axis = FIRST if ds == 0 else SECOND
        e = df if ds == 0 else ds
        for h in (0, 1):
            if e == 2:
                ag(*net, h, df, ds, 0, axis, 1, True).wait_recv()
                ag(*net, h, df, ds, 1, axis, -1, True).wait_recv()
            else:
                ag(*net, h, df, ds, "full", axis, -e, True).wait_recv()

    def onward(net, u):
        df, ds = UNITS[u]
        out = []
        if u == 0:
            for axis in (FIRST, SECOND):
                for h in (0, 1):
                    for d in (1, -1):
                        out.append((h, 0, 0, "full", axis, d))
        elif ds == 0:
            for h in (0, 1):
                if df == -1:
                    out.append((h, df, 0, 0, FIRST, 1))
                if df == 1:
                    out.append((h, df, 0, 1, FIRST, -1))
            for h in (0, 1):
                for d in (1, -1):
                    out.append((h, df, 0, "full", SECOND, d))
        elif ds != 2:
            for h in (0, 1):
                out.append((h, df, ds, 0 if ds == -1 else 1, SECOND, -ds))
        for key in out:
            c = ag(*net, *key)
            c.start()
            sent.append(c)

    sent = []
    G = (slab, ag_s, ag_r)
    L = (lbuf, lg_s, lg_r)

    own = [
        pltpu.make_async_copy(grad, slab.at[pl.ds(row * 4, 4)], cp.at[0]),
        pltpu.make_async_copy(lbas, lbuf.at[pl.ds(row * 4, 4)], cp.at[1]),
        pltpu.make_async_copy(rbas, bas.at[col], cp.at[2]),
    ]
    late = [
        pltpu.make_async_copy(rfac, acc, cp.at[3]),
        pltpu.make_async_copy(lfac, lf, cp.at[4]),
    ]
    for c in own + late:
        c.start()

    def colmate(i):
        return {"col": (col + i) % 8}

    def rowmate(i):
        return {"row": (row + i) % 16}

    barrier = pltpu.get_barrier_semaphore()

    def greet(make, n):
        def body(i, carry):
            pl.semaphore_signal(barrier, inc=1, device_id=make(i), device_id_type=MESH)
            return carry

        lax.fori_loop(1, n, body, 0)

    greet(colmate, 8)
    greet(rowmate, 16)
    for c in own:
        c.wait()
    pl.semaphore_wait(barrier, 22)

    is_k = k == z // 2
    role = (y - x + 4) % 4
    source = jnp.logical_and(is_k, role == 0)
    relay = jnp.logical_and(is_k, role != 0)
    c0 = pl.multiple_of((z % 2) * SC, 128)

    def unit_id(h, df, ds):
        return h * 16 + (df + 1) * 4 + ds + 1

    def unit_region(h, df, ds):
        return region(shared, h, df, ds, "full")

    def unit_src(h, df, ds):
        dx, dz = (df, ds) if h == 0 else (ds, df)
        return slab.at[pl.ds(rid(dx, dz) * 4 + 2 * h, 2), :, pl.ds(c0, SC)]

    def to_y(src, h, df, ds):
        i = unit_id(h, df, ds)
        return pltpu.make_async_remote_copy(
            src_ref=src, dst_ref=unit_region(h, df, ds), send_sem=y_s.at[i], recv_sem=y_r.at[i],
            device_id=ydev(1 if h == 0 else -1), device_id_type=MESH,
        )

    def to_sib(src, h, df, ds):
        i = unit_id(h, df, ds)
        return pltpu.make_async_remote_copy(
            src_ref=src, dst_ref=unit_region(h, df, ds), send_sem=sib_s.at[i], recv_sem=sib_r.at[i],
            device_id=sib, device_id_type=MESH,
        )

    def local(h, df, ds):
        return pltpu.make_async_copy(unit_src(h, df, ds), unit_region(h, df, ds), loc.at[unit_id(h, df, ds)])

    def last_role(h):
        return 3 if h == 0 else 1

    def source_unit(u):
        @pl.when(source)
        def _():
            df, ds = UNITS[u]
            for h in (0, 1):
                src = unit_src(h, df, ds)
                to_y(src, h, df, ds).start()
                to_sib(src, h, df, ds).start()
                local(h, df, ds).start()

    def hop(h):
        return role if h == 0 else (4 - role) % 4

    def relay_unit(hops, u):
        df, ds = UNITS[u]
        for h in (0, 1):

            @pl.when(jnp.logical_and(is_k, hop(h) == hops))
            def _():
                ref = unit_region(h, df, ds)
                to_y(ref, h, df, ds).wait_recv()
                if hops < 3:
                    to_y(ref, h, df, ds).start()
                to_sib(ref, h, df, ds).start()

    relayed = [0, 0, 0]

    def relay_to(hops, n):
        while relayed[hops - 1] < n:
            relay_unit(hops, relayed[hops - 1])
            relayed[hops - 1] += 1

    def b_ref(dy, kk, part):
        c = ((y + dy + 4) % 4) * 2 + kk
        return bas.at[c] if part == "full" else bas.at[c, part]

    def b_send(i, dy, part, d):
        ref = b_ref(dy, k, part)
        return pltpu.make_async_remote_copy(
            src_ref=ref, dst_ref=ref, send_sem=bs.at[i], recv_sem=br.at[i], device_id=ydev(d), device_id_type=MESH,
        )

    def b_sib(i, dy, kk):
        ref = b_ref(dy, kk, "full")
        return pltpu.make_async_remote_copy(
            src_ref=ref, dst_ref=ref, send_sem=bss.at[i], recv_sem=bsr.at[i], device_id=sib, device_id_type=MESH,
        )

    def group_ready(dx):
        units = [(0, dx, dz) for dz in (-1, 0, 1, 2)] + [(1, dz, dx) for dz in (-1, 0, 1, 2)]

        @pl.when(jnp.logical_not(is_k))
        def _():
            for u in units:
                to_sib(unit_region(*u), *u).wait_recv()

        @pl.when(source)
        def _():
            for u in units:
                local(*u).wait()

    def gram(dx, first, lo, hi):
        xg = (x + dx + 4) % 4
        rows = pl.ds(xg * 16, 16)

        for t in range(lo, hi):
            start, n = TILES[t]
            cols = pl.ds(start, n)
            a = slab[rows, :, cols].reshape(768, n)
            b = shared[rows].reshape(768, SC)
            d = lax.dot_general(a, b, (((0,), (0,)), ((), ())), preferred_element_type=F32)
            old = acc[cols, :]
            if first:
                old = ema_decay * old
            acc[cols, :] = old + (1.0 - ema_decay) * d

    def l0(yy, c):
        return pltpu.make_async_remote_copy(
            src_ref=lp.at[c], dst_ref=lsib.at[yy], send_sem=l0s.at[yy], recv_sem=l0r.at[yy],
            device_id=sib, device_id_type=MESH,
        )

    def left(dx):
        xg = (x + dx + 4) % 4

        def part(j, carry):
            c = xg * 2 + j
            a = slab[pl.ds(row * 4, 4)].reshape(192, GC)
            b = slab[pl.ds(xg * 16 + j * 8, 8)].reshape(384, GC)
            d = lax.dot_general(a, b, (((1,), (1,)), ((), ())), preferred_element_type=F32)
            lp[c] = d.astype(BF16)

            @pl.when(j != k)
            def _():
                l0(xg, c).start()

            return carry

        lax.fori_loop(0, 2, part, 0)

    def l1(dy):
        yy = (y + dy) % 4
        return pltpu.make_async_remote_copy(
            src_ref=lmid.at[yy], dst_ref=lrecv.at[y], send_sem=l1s.at[dy], recv_sem=l1r.at[dy],
            device_id={"col": yy * 2 + k}, device_id_type=MESH,
        )

    def l2(dy):
        return pltpu.make_async_remote_copy(
            src_ref=lrows.at[col], dst_ref=lrows.at[col], send_sem=l2s.at[dy], recv_sem=l2r.at[dy],
            device_id={"col": ((y + dy) % 4) * 2 + k}, device_id_type=MESH,
        )

    def l4(yy, kk):
        c = yy * 2 + kk
        return pltpu.make_async_remote_copy(
            src_ref=lrows.at[c], dst_ref=lrows.at[c], send_sem=l4s.at[yy], recv_sem=l4r.at[yy],
            device_id=sib, device_id_type=MESH,
        )

    def l3(i):
        return pltpu.make_async_remote_copy(
            src_ref=lsq.at[row], dst_ref=lsq.at[row], send_sem=l3s.at[i], recv_sem=l3r.at[i],
            device_id=rowmate(i), device_id_type=MESH,
        )

    def rq(i):
        return pltpu.make_async_remote_copy(
            src_ref=rsq.at[col], dst_ref=rsq.at[col], send_sem=q_s.at[i], recv_sem=q_r.at[i],
            device_id=colmate(i), device_id_type=MESH,
        )

    def each(n, make, what):
        def body(i, carry):
            c = make(i)
            getattr(c, what)()
            return carry

        lax.fori_loop(1, n, body, 0)

    def left_join():
        for dy in (1, 3, 2):
            yy = (y + dy) % 4
            l0(yy, yy * 2 + k).wait_recv()
            lmid[yy] = (lp[yy * 2 + k].astype(F32) + lsib[yy].astype(F32)).astype(BF16)
            l1(dy).start()

    def left_refresh():
        l0(y, col).wait_recv()
        total = lp[col].astype(F32) + lsib[y].astype(F32)
        for dy in (1, 3, 2):
            l1(dy).wait_recv()
            total = total + lrecv[(y + 4 - dy) % 4].astype(F32)
        new = ema_decay * lf[...] + (1.0 - ema_decay) * total
        ln[...] = new
        lrows[col] = new.astype(BF16)
        for dy in (1, 3, 2):
            l2(dy).start()
        l4(y, k).start()
        pltpu.make_async_copy(ln, lnew_o, cp.at[5]).start()

    def left_share():
        for dy in (1, 3, 2):
            l2(dy).wait_recv()
            l4((y + 4 - dy) % 4, k).start()

    def left_product():
        for yy in range(4):
            l4(yy, 1 - k).wait_recv()

        def part(c, carry):
            b = lbuf[pl.ds(c * 8, 8)].reshape(384, LC)
            return carry + jnp.dot(lrows[c], b, preferred_element_type=F32)

        lpr[...] = lax.fori_loop(0, 8, part, jnp.zeros((192, LC), F32))
        v = lpr[...]
        lsq[row] = jnp.broadcast_to(jnp.sum(v * v, axis=0, keepdims=True), (8, LC))
        each(16, l3, "start")
        pltpu.make_async_copy(lpr, lprod_o, cp.at[6]).start()

    def make_product(t):
        lo, n = TILES[t]
        pltpu.make_async_copy(acc.at[pl.ds(lo, n)], rnew_o.at[pl.ds(lo, n)], cp.at[8 + t]).start()

        m = PIECE[t]

        def block(cc, carry):
            half = acc[pl.ds(lo, n), :].astype(BF16)
            for e in range(4):
                xo = (x + e) % 4
                d = jnp.dot(half, bas[xo * 2 + cc].reshape(SC, 256), preferred_element_type=F32)
                for i in range(4):
                    for s in (0, 1):
                        v = d[i * m : (i + 1) * m, s * 128 : (s + 1) * 128]
                        if i >= 2:
                            both[i - 2, cc * 2 + s, xo, spot(t), :] = v.astype(BF16)
                            whole[i - 2, cc * 2 + s, xo, spot(t), :] = v
                        elif e == 2:
                            away[i, 0, cc * 2 + s, spot(t), :] = v.astype(BF16)
                        elif e == (3 if i == 0 else 1):
                            away[i, 1, cc * 2 + s, spot(t), :] = v.astype(BF16)
                        else:
                            near[i, 0 if e == 0 else 1, cc * 2 + s, spot(t), :] = v
            return carry

        lax.fori_loop(0, 2, block, 0)

    TYPES = (0, 1, 2, 3)

    def hd(i):
        return i // 2, 1 if i % 2 == 0 else -1

    def rows_of(i, t):
        return pl.ds(TILES[t][0] + i * PIECE[t], PIECE[t])

    def spot(t):
        return pl.ds(PLACE[t], PIECE[t])

    def pos(h, axis):
        return x if (h == 0) == (axis == FIRST) else z

    def parcel(i, t, kind):
        h, d = hd(i)
        if h == 0:
            return away.at[i, 0 if kind == A1 else 1, :, spot(t), :]
        return both.at[i - 2, (z + (2 if kind == A1 else -d) + 4) % 4, :, spot(t), :]

    def kept(i, t, ahead):
        h, d = hd(i)
        if h == 0:
            return near.at[i, 1 if ahead else 0, :, spot(t), :]
        return whole.at[i - 2, (z + (d if ahead else 0) + 4) % 4, :, spot(t), :]

    def rs(kind, i, t):
        h, d = hd(i)
        axis = FIRST if kind < A2 else SECOND
        q = (pos(h, SECOND) + 4) % 4
        if kind == A1:
            src, dst, to = parcel(i, t, A1), ra.at[i, :, spot(t), :], d
        elif kind == B1:
            src, dst, to = tb.at[i, :, spot(t), :], rb.at[i, :, spot(t), :], d
        elif kind == C1:
            src, dst, to = parcel(i, t, C1), rc.at[i, :, spot(t), :], -d
        elif kind == A2:
            src, dst, to = s1.at[i, (q + 2) % 4, spot(t), :], ra2.at[i, spot(t), :], d
        elif kind == B2:
            src, dst, to = tb2.at[i, spot(t), :], rb2.at[i, spot(t), :], d
        else:
            src, dst, to = s1.at[i, (q - d + 4) % 4, spot(t), :], rc2.at[i, spot(t), :], -d
        return pltpu.make_async_remote_copy(
            src_ref=src, dst_ref=dst, send_sem=rs_s.at[kind, i * 4 + t], recv_sem=rs_r.at[kind, i * 4 + t],
            device_id=neighbour(h, axis, to), device_id_type=MESH,
        )

    def r0(t):
        for kind in (A1, C1):
            for i in TYPES:
                rs(kind, i, t).start()

    def r1(t):
        for i in TYPES:
            h, d = hd(i)
            rs(A1, i, t).wait_recv()
            tb[i, :, spot(t), :] = (kept(i, t, True)[...] + ra[i, :, spot(t), :].astype(F32)).astype(BF16)
            rs(B1, i, t).start()

    def r2(t):
        for i in TYPES:
            h, d = hd(i)
            rs(C1, i, t).wait_recv()
            rs(B1, i, t).wait_recv()
            total = kept(i, t, False)[...] + rb[i, :, spot(t), :].astype(F32) + rc[i, :, spot(t), :].astype(F32)
            s1[i, :, spot(t), :] = total.astype(BF16)
            rs(A2, i, t).start()
            rs(C2, i, t).start()
            q = pos(h, SECOND)
            for f, e in ((0, 0), (1, d)):
                w = (q + e + 4) % 4
                mine = kept(i, t, False).at[w]
                keep[f, i, spot(t), :] = (
                    mine[...] + rb[i, w, spot(t), :].astype(F32) + rc[i, w, spot(t), :].astype(F32)
                )

    def r3(t):
        for i in TYPES:
            h, d = hd(i)
            rs(A2, i, t).wait_recv()
            tb2[i, spot(t), :] = (keep[1, i, spot(t), :] + ra2[i, spot(t), :].astype(F32)).astype(BF16)
            rs(B2, i, t).start()

    def r4(t):
        total = jnp.zeros((8, 128), F32)
        for i in TYPES:
            rs(C2, i, t).wait_recv()
            rs(B2, i, t).wait_recv()
            v = keep[0, i, spot(t), :] + rb2[i, spot(t), :].astype(F32) + rc2[i, spot(t), :].astype(F32)
            rout[rows_of(i, t), :] = v
            total = total + jnp.sum((v * v).reshape(PIECE[t] // 8, 8, 128), axis=0)
        lo, n = TILES[t]
        pltpu.make_async_copy(rout.at[pl.ds(lo, n)], rprod_o.at[pl.ds(lo, n)], cp.at[12 + t]).start()
        return total

    H = (0, 1)
    b_sends, b_sibs = [], []

    def begin(send, sibs):
        for c in send + sibs:
            c.start()
        b_sends.extend(send)
        b_sibs.extend(sibs)

    def lb(a, b):
        for u in range(a, b):
            arrive(L, u)
            onward(L, u)

    for u in range(16):
        arrive(G, u)
        onward(G, u)
        source_unit(u)
        for hops in (1, 2, 3):
            relay_to(hops, u + 1 - LAGS[hops - 1])
        if u == 2:
            begin([b_send(0, 0, "full", 1), b_send(1, 0, "full", -1)], [b_sib(0, 0, k)])
        if u == 8:
            b_send(0, -1, "full", 1).wait_recv()
            b_send(1, 1, "full", -1).wait_recv()
            begin([b_send(2, -1, 0, 1), b_send(3, 1, 1, -1)], [b_sib(1, -1, k), b_sib(2, 1, k)])
        if u == 12:
            onward(L, 0)
        if u == 15:
            lb(1, 3)
        if u == 14:
            late[0].wait()
            relay_to(3, 11)
            group_ready(0)
            gram(0, True, 0, 4)
    relay_to(1, 16)
    lb(3, 6)
    relay_to(2, 16)
    b_send(2, 2, 0, 1).wait_recv()
    b_send(3, 2, 1, -1).wait_recv()
    begin([], [b_sib(3, 2, k)])

    relay_to(3, 14)
    group_ready(-1)
    gram(-1, False, 0, 4)
    lb(6, 10)
    relay_to(3, 15)
    group_ready(1)
    gram(1, False, 0, 4)
    relay_to(3, 16)
    for i, dy in enumerate((0, -1, 1, 2)):
        b_sib(i, dy, 1 - k).wait_recv()
    group_ready(2)
    gram(2, False, 0, 1)
    make_product(0)
    r0(0)
    lb(10, 13)
    gram(2, False, 1, 2)
    make_product(1)
    r0(1)
    for dx in (0, -1, 1, 2):
        left(dx)
    r1(0)
    gram(2, False, 2, 3)
    make_product(2)
    r0(2)
    left_join()
    r1(1)
    gram(2, False, 3, 4)
    make_product(3)
    r0(3)
    r1(2)
    lb(13, 16)
    r2(0)
    late[1].wait()
    left_refresh()
    r1(3)
    r3(0)
    r2(1)
    total = r4(0)
    left_share()
    r3(1)
    r2(2)
    total = total + r4(1)
    left_product()
    r3(2)
    r2(3)
    total = total + r4(2)
    r3(3)
    total = total + r4(3)
    rsq[col] = total
    each(8, rq, "start")

    each(16, l3, "wait_recv")
    lsum = pltpu.make_async_copy(lsq, lsum_o, cp.at[7])
    lsum.start()
    each(8, rq, "wait_recv")
    rsum = pltpu.make_async_copy(rsq, rsum_o, cp.at[16])
    rsum.start()

    for c in sent + b_sends + b_sibs:
        c.wait_send()
    for df, ds in UNITS:
        for h in H:
            ref = unit_region(h, df, ds)

            @pl.when(jnp.logical_and(is_k, hop(h) != 3))
            def _():
                to_y(ref, h, df, ds).wait_send()

            @pl.when(is_k)
            def _():
                to_sib(ref, h, df, ds).wait_send()

    for kind in range(6):
        for i in TYPES:
            for t in range(4):
                rs(kind, i, t).wait_send()
    for yy in range(4):
        l0(yy, yy * 2 + 1 - k).wait_send()
        l4(yy, k).wait_send()
    for dy in (1, 2, 3):
        l1(dy).wait_send()
        l2(dy).wait_send()
    each(16, l3, "wait_send")
    each(8, rq, "wait_send")
    for t, (lo, n) in enumerate(TILES):
        pltpu.make_async_copy(acc.at[pl.ds(lo, n)], rnew_o.at[pl.ds(lo, n)], cp.at[8 + t]).wait()
        pltpu.make_async_copy(rout.at[pl.ds(lo, n)], rprod_o.at[pl.ds(lo, n)], cp.at[12 + t]).wait()
    pltpu.make_async_copy(ln, lnew_o, cp.at[5]).wait()
    pltpu.make_async_copy(lpr, lprod_o, cp.at[6]).wait()
    lsum.wait()
    rsum.wait()


def refresh(gradient, left_basis, right_basis, right_factor, left_factor):
    dma = pltpu.SemaphoreType.DMA
    n = len(AG)
    any_spec = pl.BlockSpec(memory_space=pl.ANY)
    V = pltpu.VMEM
    return pl.pallas_call(
        kernel,
        out_shape=(
            jax.ShapeDtypeStruct((GC, SC), F32),
            jax.ShapeDtypeStruct((GC, 128), F32),
            jax.ShapeDtypeStruct((8, 8, 128), F32),
            jax.ShapeDtypeStruct((192, LC), F32),
            jax.ShapeDtypeStruct((192, LC), F32),
            jax.ShapeDtypeStruct((16, 8, LC), F32),
        ),
        in_specs=[any_spec] * 5,
        out_specs=[any_spec] * 6,
        scratch_shapes=[
            V((64, 48, GC), BF16), V((64, 48, LC), BF16), V((64, 48, SC), BF16), V((GC, SC), F32),
            V((8, 2, 448, 256), BF16), V((8, 192, LC), BF16),
            V((2, 2, 4, 448, 128), BF16), V((2, 2, 4, 448, 128), F32),
            V((2, 4, 4, 448, 128), BF16), V((2, 4, 4, 448, 128), F32),
            V((4, 4, 448, 128), BF16), V((4, 4, 448, 128), BF16), V((4, 4, 448, 128), BF16),
            V((4, 4, 448, 128), BF16), V((4, 4, 448, 128), BF16), V((2, 4, 448, 128), F32),
            V((4, 448, 128), BF16), V((4, 448, 128), BF16), V((4, 448, 128), BF16), V((4, 448, 128), BF16),
            V((GC, 128), F32), V((8, 8, 128), F32),
            V((4, 192, LC), BF16), V((4, 192, LC), BF16), V((4, 192, LC), BF16), V((8, 192, LC), BF16),
            V((192, LC), F32), V((192, LC), F32), V((192, LC), F32), V((16, 8, LC), F32),
            dma((n,)), dma((n,)), dma((n,)), dma((n,)),
            dma((32,)), dma((32,)), dma((32,)), dma((32,)), dma((32,)),
            dma((4,)), dma((4,)), dma((4,)), dma((4,)), dma((17,)),
            dma((6, 16)), dma((6, 16)),
            dma((4,)), dma((4,)), dma((4,)), dma((4,)), dma((4,)), dma((4,)), dma((4,)), dma((4,)),
            dma((16,)), dma((16,)), dma((8,)), dma((8,)),
        ],
        compiler_params=pltpu.CompilerParams(
            collective_id=0, has_side_effects=True, vmem_limit_bytes=67043328
        ),
        name="refresh",
    )(
        gradient.reshape(4, 48, GC), left_basis.reshape(4, 48, LC), right_basis.reshape(2, 448, 256),
        right_factor, left_factor,
    )


def finish_kernel(rnew, rprod, rsq, lnew, lprod, lsq, lnew_o, rnew_o, lout_o, rout_o):
    rnew_o[...] = rnew[...]
    right_sq = jnp.sum(rsq[...].reshape(64, 128), axis=0, keepdims=True)
    rout_o[...] = rprod[...] * lax.rsqrt(right_sq / DHIDDEN + epsilon)

    @pl.when(pl.program_id(0) == 0)
    def _():
        lnew_o[...] = lnew[...]
        left_sq = jnp.sum(lsq[...], axis=0)[:1]
        lout_o[...] = lprod[...] * lax.rsqrt(left_sq / DMODEL + epsilon)


def finish(right_new, right_prod, rsq, left_new, left_prod, lsq):
    def rows(n):
        return pl.BlockSpec((448, n), lambda i: (i, 0))

    def whole(*shape):
        return pl.BlockSpec(shape, lambda i: (0,) * len(shape))

    return pl.pallas_call(
        finish_kernel,
        grid=(4,),
        out_shape=(
            jax.ShapeDtypeStruct((192, LC), F32),
            jax.ShapeDtypeStruct((GC, SC), F32),
            jax.ShapeDtypeStruct((192, LC), F32),
            jax.ShapeDtypeStruct((GC, 128), F32),
        ),
        in_specs=[rows(SC), rows(128), whole(8, 8, 128), whole(192, LC), whole(192, LC), whole(16, 8, LC)],
        out_specs=(whole(192, LC), rows(SC), whole(192, LC), rows(128)),
        compiler_params=pltpu.CompilerParams(vmem_limit_bytes=60 * 1024 * 1024),
        name="finish",
    )(right_new, right_prod, rsq, left_new, left_prod, lsq)


def on_device(gradient, left_factor, right_factor, left_basis, right_basis):
    return finish(*refresh(gradient, left_basis, right_basis, right_factor, left_factor))


def solution(mesh):
    in_specs = (P("row", "col"), P("row", "col"), P("col", "row"), P("row", "col"), P("row", "col"))
    out_specs = (P("row", "col"), P("col", "row"), P("row", "col"), P("col", "row"))
    return jax.shard_map(on_device, mesh=mesh, in_specs=in_specs, out_specs=out_specs, check_vma=False)
```

```python
import functools

import jax
import jax.numpy as jnp
from jax import lax
from jax.experimental import pallas as pl
from jax.experimental.pallas import tpu as pltpu
from jax.sharding import PartitionSpec as P

DMODEL = 3072
DHIDDEN = 14336
ema_decay = 0.95
epsilon = 1e-06
MESH = pl.DeviceIdType.MESH
F32 = jnp.float32
BF16 = jnp.bfloat16
GC = 1792
LC = 384
SC = 896
FIRST, SECOND = "f", "s"
TILES = ((0, 512), (512, 512), (1024, 512), (1536, 256))
PIECE = [n // 4 for _, n in TILES]
PLACE = [sum(PIECE[:t]) for t in range(len(TILES))]
A1, B1, C1, A2, B2, C2 = range(6)


def wrap(v):
    return (v + 1) % 4 - 1


def message_table():
    keys = []
    for h in (0, 1):
        for axis in (FIRST, SECOND):
            for d in (1, -1):
                keys.append((h, 0, 0, "full", axis, d))
        keys.append((h, -1, 0, 0, FIRST, 1))
        keys.append((h, 1, 0, 1, FIRST, -1))
        for df in (-1, 1, 2):
            for d in (1, -1):
                keys.append((h, df, 0, "full", SECOND, d))
        for df in (0, -1, 1, 2):
            keys.append((h, df, -1, 0, SECOND, 1))
            keys.append((h, df, 1, 1, SECOND, -1))
    return {key: i for i, key in enumerate(keys)}


AG = message_table()
UNITS = [
    (0, 0), (-1, 0), (1, 0), (0, -1), (0, 1), (2, 0), (-1, -1), (-1, 1), (1, -1), (1, 1),
    (0, 2), (2, -1), (2, 1), (-1, 2), (1, 2), (2, 2),
]
LAGS = (1, 2, 4)


def kernel(
    grad, lbas, rbas, rfac, lfac,
    acc, rout, rsum, ln, lpr, lsum,
    slab, lbuf, shared, bas, lp, away, near, both, whole,
    ra, tb, rb, rc, s1, keep, ra2, tb2, rb2, rc2, rsq,
    lsib, lmid, lrecv, lrows, lf, lsq,
    ag_s, ag_r, lg_s, lg_r, y_s, y_r, sib_s, sib_r, loc, bs, br, bss, bsr, cp,
    rs_s, rs_r, l0s, l0r, l1s, l1r, l2s, l2r, l4s, l4r, l3s, l3r, q_s, q_r,
):
    row = lax.axis_index("row")
    col = lax.axis_index("col")
    x, z = row // 4, row % 4
    y, k = col // 2, col % 2
    sib = {"col": y * 2 + (1 - k)}

    def ydev(d):
        return {"col": ((y + d + 4) % 4) * 2 + k}

    def rid(dx, dz):
        return ((x + dx + 4) % 4) * 4 + (z + dz + 4) % 4

    def region(ref, h, df, ds, part):
        dx, dz = (df, ds) if h == 0 else (ds, df)
        q, n = (0, 2) if part == "full" else (part, 1)
        return ref.at[pl.ds(rid(dx, dz) * 4 + 2 * h + q, n)]

    def neighbour(h, axis, d):
        if (h == 0) == (axis == FIRST):
            return {"row": ((x + d + 4) % 4) * 4 + z}
        return {"row": x * 4 + (z + d + 4) % 4}

    def ag(buf, ss, rr, h, df, ds, part, axis, d, arriving=False):
        if not arriving:
            key = (h, df, ds, part, axis, d)
        elif axis == FIRST:
            key = (h, wrap(df + d), ds, part, axis, d)
        else:
            key = (h, df, wrap(ds + d), part, axis, d)
        i = AG[key]
        ref = region(buf, h, df, ds, part)
        return pltpu.make_async_remote_copy(
            src_ref=ref, dst_ref=ref, send_sem=ss.at[i], recv_sem=rr.at[i],
            device_id=neighbour(h, axis, d), device_id_type=MESH,
        )

    def arrive(net, u):
        df, ds = UNITS[u]
        if u == 0:
            return
        axis = FIRST if ds == 0 else SECOND
        e = df if ds == 0 else ds
        for h in (0, 1):
            if e == 2:
                ag(*net, h, df, ds, 0, axis, 1, True).wait_recv()
                ag(*net, h, df, ds, 1, axis, -1, True).wait_recv()
            else:
                ag(*net, h, df, ds, "full", axis, -e, True).wait_recv()

    def onward(net, u):
        df, ds = UNITS[u]
        out = []
        if u == 0:
            for axis in (FIRST, SECOND):
                for h in (0, 1):
                    for d in (1, -1):
                        out.append((h, 0, 0, "full", axis, d))
        elif ds == 0:
            for h in (0, 1):
                if df == -1:
                    out.append((h, df, 0, 0, FIRST, 1))
                if df == 1:
                    out.append((h, df, 0, 1, FIRST, -1))
            for h in (0, 1):
                for d in (1, -1):
                    out.append((h, df, 0, "full", SECOND, d))
        elif ds != 2:
            for h in (0, 1):
                out.append((h, df, ds, 0 if ds == -1 else 1, SECOND, -ds))
        for key in out:
            c = ag(*net, *key)
            c.start()
            sent.append(c)

    sent = []
    G = (slab, ag_s, ag_r)
    L = (lbuf, lg_s, lg_r)

    own = [
        pltpu.make_async_copy(grad, slab.at[pl.ds(row * 4, 4)], cp.at[0]),
        pltpu.make_async_copy(lbas, lbuf.at[pl.ds(row * 4, 4)], cp.at[1]),
        pltpu.make_async_copy(rbas, bas.at[col], cp.at[2]),
    ]
    late = [
        pltpu.make_async_copy(rfac, acc, cp.at[3]),
        pltpu.make_async_copy(lfac, lf, cp.at[4]),
    ]
    for c in own + late:
        c.start()

    def colmate(i):
        return {"col": (col + i) % 8}

    def rowmate(i):
        return {"row": (row + i) % 16}

    barrier = pltpu.get_barrier_semaphore()

    def greet(make, n):
        def body(i, carry):
            pl.semaphore_signal(barrier, inc=1, device_id=make(i), device_id_type=MESH)
            return carry

        lax.fori_loop(1, n, body, 0)

    greet(colmate, 8)
    greet(rowmate, 16)
    for c in own:
        c.wait()
    pl.semaphore_wait(barrier, 22)

    is_k = k == z // 2
    role = (y - x + 4) % 4
    source = jnp.logical_and(is_k, role == 0)
    relay = jnp.logical_and(is_k, role != 0)
    c0 = pl.multiple_of((z % 2) * SC, 128)

    def unit_id(h, df, ds):
        return h * 16 + (df + 1) * 4 + ds + 1

    def unit_region(h, df, ds):
        return region(shared, h, df, ds, "full")

    def unit_src(h, df, ds):
        dx, dz = (df, ds) if h == 0 else (ds, df)
        return slab.at[pl.ds(rid(dx, dz) * 4 + 2 * h, 2), :, pl.ds(c0, SC)]

    def to_y(src, h, df, ds):
        i = unit_id(h, df, ds)
        return pltpu.make_async_remote_copy(
            src_ref=src, dst_ref=unit_region(h, df, ds), send_sem=y_s.at[i], recv_sem=y_r.at[i],
            device_id=ydev(1 if h == 0 else -1), device_id_type=MESH,
        )

    def to_sib(src, h, df, ds):
        i = unit_id(h, df, ds)
        return pltpu.make_async_remote_copy(
            src_ref=src, dst_ref=unit_region(h, df, ds), send_sem=sib_s.at[i], recv_sem=sib_r.at[i],
            device_id=sib, device_id_type=MESH,
        )

    def local(h, df, ds):
        return pltpu.make_async_copy(unit_src(h, df, ds), unit_region(h, df, ds), loc.at[unit_id(h, df, ds)])

    def last_role(h):
        return 3 if h == 0 else 1

    def source_unit(u):
        @pl.when(source)
        def _():
            df, ds = UNITS[u]
            for h in (0, 1):
                src = unit_src(h, df, ds)
                to_y(src, h, df, ds).start()
                to_sib(src, h, df, ds).start()
                local(h, df, ds).start()

    def hop(h):
        return role if h == 0 else (4 - role) % 4

    def relay_unit(hops, u):
        df, ds = UNITS[u]
        for h in (0, 1):

            @pl.when(jnp.logical_and(is_k, hop(h) == hops))
            def _():
                ref = unit_region(h, df, ds)
                to_y(ref, h, df, ds).wait_recv()
                if hops < 3:
                    to_y(ref, h, df, ds).start()
                to_sib(ref, h, df, ds).start()

    relayed = [0, 0, 0]

    def relay_to(hops, n):
        while relayed[hops - 1] < n:
            relay_unit(hops, relayed[hops - 1])
            relayed[hops - 1] += 1

    def b_ref(dy, kk, part):
        c = ((y + dy + 4) % 4) * 2 + kk
        return bas.at[c] if part == "full" else bas.at[c, part]

    def b_send(i, dy, part, d):
        ref = b_ref(dy, k, part)
        return pltpu.make_async_remote_copy(
            src_ref=ref, dst_ref=ref, send_sem=bs.at[i], recv_sem=br.at[i], device_id=ydev(d), device_id_type=MESH,
        )

    def b_sib(i, dy, kk):
        ref = b_ref(dy, kk, "full")
        return pltpu.make_async_remote_copy(
            src_ref=ref, dst_ref=ref, send_sem=bss.at[i], recv_sem=bsr.at[i], device_id=sib, device_id_type=MESH,
        )

    def group_ready(dx):
        units = [(0, dx, dz) for dz in (-1, 0, 1, 2)] + [(1, dz, dx) for dz in (-1, 0, 1, 2)]

        @pl.when(jnp.logical_not(is_k))
        def _():
            for u in units:
                to_sib(unit_region(*u), *u).wait_recv()

        @pl.when(source)
        def _():
            for u in units:
                local(*u).wait()

    def gram(dx, first, lo, hi):
        xg = (x + dx + 4) % 4
        rows = pl.ds(xg * 16, 16)

        for t in range(lo, hi):
            start, n = TILES[t]
            cols = pl.ds(start, n)
            a = slab[rows, :, cols].reshape(768, n)
            b = shared[rows].reshape(768, SC)
            d = lax.dot_general(a, b, (((0,), (0,)), ((), ())), preferred_element_type=F32)
            old = acc[cols, :]
            if first:
                old = ema_decay * old
            acc[cols, :] = old + (1.0 - ema_decay) * d

    def l0(yy, c):
        return pltpu.make_async_remote_copy(
            src_ref=lp.at[c], dst_ref=lsib.at[yy], send_sem=l0s.at[yy], recv_sem=l0r.at[yy],
            device_id=sib, device_id_type=MESH,
        )

    def left(dx):
        xg = (x + dx + 4) % 4

        def part(j, carry):
            c = xg * 2 + j
            a = slab[pl.ds(row * 4, 4)].reshape(192, GC)
            b = slab[pl.ds(xg * 16 + j * 8, 8)].reshape(384, GC)
            d = lax.dot_general(a, b, (((1,), (1,)), ((), ())), preferred_element_type=F32)
            lp[c] = d.astype(BF16)

            @pl.when(j != k)
            def _():
                l0(xg, c).start()

            return carry

        lax.fori_loop(0, 2, part, 0)

    def l1(dy):
        yy = (y + dy) % 4
        return pltpu.make_async_remote_copy(
            src_ref=lmid.at[yy], dst_ref=lrecv.at[y], send_sem=l1s.at[dy], recv_sem=l1r.at[dy],
            device_id={"col": yy * 2 + k}, device_id_type=MESH,
        )

    def l2(dy):
        return pltpu.make_async_remote_copy(
            src_ref=lrows.at[col], dst_ref=lrows.at[col], send_sem=l2s.at[dy], recv_sem=l2r.at[dy],
            device_id={"col": ((y + dy) % 4) * 2 + k}, device_id_type=MESH,
        )

    def l4(yy, kk):
        c = yy * 2 + kk
        return pltpu.make_async_remote_copy(
            src_ref=lrows.at[c], dst_ref=lrows.at[c], send_sem=l4s.at[yy], recv_sem=l4r.at[yy],
            device_id=sib, device_id_type=MESH,
        )

    def l3(i):
        return pltpu.make_async_remote_copy(
            src_ref=lsq.at[row], dst_ref=lsq.at[row], send_sem=l3s.at[i], recv_sem=l3r.at[i],
            device_id=rowmate(i), device_id_type=MESH,
        )

    def rq(i):
        return pltpu.make_async_remote_copy(
            src_ref=rsq.at[col], dst_ref=rsq.at[col], send_sem=q_s.at[i], recv_sem=q_r.at[i],
            device_id=colmate(i), device_id_type=MESH,
        )

    def each(n, make, what):
        def body(i, carry):
            c = make(i)
            getattr(c, what)()
            return carry

        lax.fori_loop(1, n, body, 0)

    def left_join():
        for dy in (1, 3, 2):
            yy = (y + dy) % 4
            l0(yy, yy * 2 + k).wait_recv()
            lmid[yy] = (lp[yy * 2 + k].astype(F32) + lsib[yy].astype(F32)).astype(BF16)
            l1(dy).start()

    def left_refresh():
        l0(y, col).wait_recv()
        total = lp[col].astype(F32) + lsib[y].astype(F32)
        for dy in (1, 3, 2):
            l1(dy).wait_recv()
            total = total + lrecv[(y + 4 - dy) % 4].astype(F32)
        new = ema_decay * lf[...] + (1.0 - ema_decay) * total
        ln[...] = new
        lrows[col] = new.astype(BF16)
        for dy in (1, 3, 2):
            l2(dy).start()
        l4(y, k).start()

    def left_share():
        for dy in (1, 3, 2):
            l2(dy).wait_recv()
            l4((y + 4 - dy) % 4, k).start()

    def left_product():
        for yy in range(4):
            l4(yy, 1 - k).wait_recv()

        def part(c, carry):
            b = lbuf[pl.ds(c * 8, 8)].reshape(384, LC)
            return carry + jnp.dot(lrows[c], b, preferred_element_type=F32)

        lpr[...] = lax.fori_loop(0, 8, part, jnp.zeros((192, LC), F32))
        v = lpr[...]
        lsq[row] = jnp.broadcast_to(jnp.sum(v * v, axis=0, keepdims=True), (8, LC))
        each(16, l3, "start")

    def make_product(t):
        lo, n = TILES[t]

        m = PIECE[t]

        def block(cc, carry):
            half = acc[pl.ds(lo, n), :].astype(BF16)
            for e in range(4):
                xo = (x + e) % 4
                d = jnp.dot(half, bas[xo * 2 + cc].reshape(SC, 256), preferred_element_type=F32)
                for i in range(4):
                    for s in (0, 1):
                        v = d[i * m : (i + 1) * m, s * 128 : (s + 1) * 128]
                        if i >= 2:
                            both[i - 2, cc * 2 + s, xo, spot(t), :] = v.astype(BF16)
                            whole[i - 2, cc * 2 + s, xo, spot(t), :] = v
                        elif e == 2:
                            away[i, 0, cc * 2 + s, spot(t), :] = v.astype(BF16)
                        elif e == (3 if i == 0 else 1):
                            away[i, 1, cc * 2 + s, spot(t), :] = v.astype(BF16)
                        else:
                            near[i, 0 if e == 0 else 1, cc * 2 + s, spot(t), :] = v
            return carry

        lax.fori_loop(0, 2, block, 0)

    TYPES = (0, 1, 2, 3)

    def hd(i):
        return i // 2, 1 if i % 2 == 0 else -1

    def rows_of(i, t):
        return pl.ds(TILES[t][0] + i * PIECE[t], PIECE[t])

    def spot(t):
        return pl.ds(PLACE[t], PIECE[t])

    def pos(h, axis):
        return x if (h == 0) == (axis == FIRST) else z

    def parcel(i, t, kind):
        h, d = hd(i)
        if h == 0:
            return away.at[i, 0 if kind == A1 else 1, :, spot(t), :]
        return both.at[i - 2, (z + (2 if kind == A1 else -d) + 4) % 4, :, spot(t), :]

    def kept(i, t, ahead):
        h, d = hd(i)
        if h == 0:
            return near.at[i, 1 if ahead else 0, :, spot(t), :]
        return whole.at[i - 2, (z + (d if ahead else 0) + 4) % 4, :, spot(t), :]

    def rs(kind, i, t):
        h, d = hd(i)
        axis = FIRST if kind < A2 else SECOND
        q = (pos(h, SECOND) + 4) % 4
        if kind == A1:
            src, dst, to = parcel(i, t, A1), ra.at[i, :, spot(t), :], d
        elif kind == B1:
            src, dst, to = tb.at[i, :, spot(t), :], rb.at[i, :, spot(t), :], d
        elif kind == C1:
            src, dst, to = parcel(i, t, C1), rc.at[i, :, spot(t), :], -d
        elif kind == A2:
            src, dst, to = s1.at[i, (q + 2) % 4, spot(t), :], ra2.at[i, spot(t), :], d
        elif kind == B2:
            src, dst, to = tb2.at[i, spot(t), :], rb2.at[i, spot(t), :], d
        else:
            src, dst, to = s1.at[i, (q - d + 4) % 4, spot(t), :], rc2.at[i, spot(t), :], -d
        return pltpu.make_async_remote_copy(
            src_ref=src, dst_ref=dst, send_sem=rs_s.at[kind, i * 4 + t], recv_sem=rs_r.at[kind, i * 4 + t],
            device_id=neighbour(h, axis, to), device_id_type=MESH,
        )

    def r0(t):
        for kind in (A1, C1):
            for i in TYPES:
                rs(kind, i, t).start()

    def r1(t):
        for i in TYPES:
            h, d = hd(i)
            rs(A1, i, t).wait_recv()
            tb[i, :, spot(t), :] = (kept(i, t, True)[...] + ra[i, :, spot(t), :].astype(F32)).astype(BF16)
            rs(B1, i, t).start()

    def r2(t):
        for i in TYPES:
            h, d = hd(i)
            rs(C1, i, t).wait_recv()
            rs(B1, i, t).wait_recv()
            total = kept(i, t, False)[...] + rb[i, :, spot(t), :].astype(F32) + rc[i, :, spot(t), :].astype(F32)
            s1[i, :, spot(t), :] = total.astype(BF16)
            rs(A2, i, t).start()
            rs(C2, i, t).start()
            q = pos(h, SECOND)
            for f, e in ((0, 0), (1, d)):
                w = (q + e + 4) % 4
                mine = kept(i, t, False).at[w]
                keep[f, i, spot(t), :] = (
                    mine[...] + rb[i, w, spot(t), :].astype(F32) + rc[i, w, spot(t), :].astype(F32)
                )

    def r3(t):
        for i in TYPES:
            h, d = hd(i)
            rs(A2, i, t).wait_recv()
            tb2[i, spot(t), :] = (keep[1, i, spot(t), :] + ra2[i, spot(t), :].astype(F32)).astype(BF16)
            rs(B2, i, t).start()

    def r4(t):
        total = jnp.zeros((8, 128), F32)
        for i in TYPES:
            rs(C2, i, t).wait_recv()
            rs(B2, i, t).wait_recv()
            v = keep[0, i, spot(t), :] + rb2[i, spot(t), :].astype(F32) + rc2[i, spot(t), :].astype(F32)
            rout[rows_of(i, t), :] = v
            total = total + jnp.sum((v * v).reshape(PIECE[t] // 8, 8, 128), axis=0)
        return total

    H = (0, 1)
    b_sends, b_sibs = [], []

    def begin(send, sibs):
        for c in send + sibs:
            c.start()
        b_sends.extend(send)
        b_sibs.extend(sibs)

    def lb(a, b):
        for u in range(a, b):
            arrive(L, u)
            onward(L, u)

    for u in range(16):
        arrive(G, u)
        onward(G, u)
        source_unit(u)
        for hops in (1, 2, 3):
            relay_to(hops, u + 1 - LAGS[hops - 1])
        if u == 2:
            begin([b_send(0, 0, "full", 1), b_send(1, 0, "full", -1)], [b_sib(0, 0, k)])
        if u == 8:
            b_send(0, -1, "full", 1).wait_recv()
            b_send(1, 1, "full", -1).wait_recv()
            begin([b_send(2, -1, 0, 1), b_send(3, 1, 1, -1)], [b_sib(1, -1, k), b_sib(2, 1, k)])
        if u == 12:
            onward(L, 0)
        if u == 15:
            lb(1, 3)
        if u == 14:
            late[0].wait()
            relay_to(3, 11)
            group_ready(0)
            gram(0, True, 0, 4)
    relay_to(1, 16)
    lb(3, 6)
    relay_to(2, 16)
    b_send(2, 2, 0, 1).wait_recv()
    b_send(3, 2, 1, -1).wait_recv()
    begin([], [b_sib(3, 2, k)])

    relay_to(3, 14)
    group_ready(-1)
    gram(-1, False, 0, 4)
    lb(6, 10)
    relay_to(3, 15)
    group_ready(1)
    gram(1, False, 0, 4)
    relay_to(3, 16)
    for i, dy in enumerate((0, -1, 1, 2)):
        b_sib(i, dy, 1 - k).wait_recv()
    group_ready(2)
    gram(2, False, 0, 1)
    make_product(0)
    r0(0)
    lb(10, 13)
    gram(2, False, 1, 2)
    make_product(1)
    r0(1)
    for dx in (0, -1, 1, 2):
        left(dx)
    r1(0)
    gram(2, False, 2, 3)
    make_product(2)
    r0(2)
    left_join()
    r1(1)
    gram(2, False, 3, 4)
    make_product(3)
    r0(3)
    r1(2)
    lb(13, 16)
    r2(0)
    late[1].wait()
    left_refresh()
    r1(3)
    r3(0)
    r2(1)
    total = r4(0)
    left_share()
    r3(1)
    r2(2)
    total = total + r4(1)
    left_product()
    r3(2)
    r2(3)
    total = total + r4(2)
    r3(3)
    total = total + r4(3)
    rsq[col] = total
    each(8, rq, "start")

    each(16, l3, "wait_recv")
    lsum[...] = jnp.sum(lsq[...], axis=0)
    each(8, rq, "wait_recv")
    rsum[...] = jnp.sum(rsq[...], axis=0)

    for c in sent + b_sends + b_sibs:
        c.wait_send()
    for df, ds in UNITS:
        for h in H:
            ref = unit_region(h, df, ds)

            @pl.when(jnp.logical_and(is_k, hop(h) != 3))
            def _():
                to_y(ref, h, df, ds).wait_send()

            @pl.when(is_k)
            def _():
                to_sib(ref, h, df, ds).wait_send()

    for kind in range(6):
        for i in TYPES:
            for t in range(4):
                rs(kind, i, t).wait_send()
    for yy in range(4):
        l0(yy, yy * 2 + 1 - k).wait_send()
        l4(yy, k).wait_send()
    for dy in (1, 2, 3):
        l1(dy).wait_send()
        l2(dy).wait_send()
    each(16, l3, "wait_send")
    each(8, rq, "wait_send")


def refresh(gradient, left_basis, right_basis, right_factor, left_factor):
    dma = pltpu.SemaphoreType.DMA
    n = len(AG)
    any_spec = pl.BlockSpec(memory_space=pl.ANY)
    V = pltpu.VMEM
    return pl.pallas_call(
        kernel,
        out_shape=(
            V((GC, SC), F32),
            V((GC, 128), F32),
            V((8, 128), F32),
            V((192, LC), F32),
            V((192, LC), F32),
            V((8, LC), F32),
        ),
        in_specs=[any_spec] * 5,
        out_specs=[pl.BlockSpec(memory_space=pltpu.VMEM)] * 6,
        scratch_shapes=[
            V((64, 48, GC), BF16), V((64, 48, LC), BF16), V((64, 48, SC), BF16),
            V((8, 2, 448, 256), BF16), V((8, 192, LC), BF16),
            V((2, 2, 4, 448, 128), BF16), V((2, 2, 4, 448, 128), F32),
            V((2, 4, 4, 448, 128), BF16), V((2, 4, 4, 448, 128), F32),
            V((4, 4, 448, 128), BF16), V((4, 4, 448, 128), BF16), V((4, 4, 448, 128), BF16),
            V((4, 4, 448, 128), BF16), V((4, 4, 448, 128), BF16), V((2, 4, 448, 128), F32),
            V((4, 448, 128), BF16), V((4, 448, 128), BF16), V((4, 448, 128), BF16), V((4, 448, 128), BF16),
            V((8, 8, 128), F32),
            V((4, 192, LC), BF16), V((4, 192, LC), BF16), V((4, 192, LC), BF16), V((8, 192, LC), BF16),
            V((192, LC), F32), V((16, 8, LC), F32),
            dma((n,)), dma((n,)), dma((n,)), dma((n,)),
            dma((32,)), dma((32,)), dma((32,)), dma((32,)), dma((32,)),
            dma((4,)), dma((4,)), dma((4,)), dma((4,)), dma((5,)),
            dma((6, 16)), dma((6, 16)),
            dma((4,)), dma((4,)), dma((4,)), dma((4,)), dma((4,)), dma((4,)), dma((4,)), dma((4,)),
            dma((16,)), dma((16,)), dma((8,)), dma((8,)),
        ],
        compiler_params=pltpu.CompilerParams(
            collective_id=0, has_side_effects=True, vmem_limit_bytes=58800000
        ),
        name="refresh",
    )(
        gradient.reshape(4, 48, GC), left_basis.reshape(4, 48, LC), right_basis.reshape(2, 448, 256),
        right_factor, left_factor,
    )


def finish_kernel(rnew, rprod, rsum, lnew, lprod, lsum, lnew_o, rnew_o, lout_o, rout_o, rout, lout, sem):
    copies = [pltpu.make_async_copy(rnew, rnew_o, sem.at[0]), pltpu.make_async_copy(lnew, lnew_o, sem.at[1])]
    for c in copies:
        c.start()
    right_sq = jnp.sum(rsum[...], axis=0, keepdims=True)
    rout[...] = rprod[...] * lax.rsqrt(right_sq / DHIDDEN + epsilon)
    copies.append(pltpu.make_async_copy(rout, rout_o, sem.at[2]))
    copies[2].start()
    lout[...] = lprod[...] * lax.rsqrt(lsum[:1, :] / DMODEL + epsilon)
    copies.append(pltpu.make_async_copy(lout, lout_o, sem.at[3]))
    copies[3].start()
    for c in copies:
        c.wait()


def finish(*results):
    vmem = pl.BlockSpec(memory_space=pltpu.VMEM)
    return pl.pallas_call(
        finish_kernel,
        out_shape=(
            jax.ShapeDtypeStruct((192, LC), F32),
            jax.ShapeDtypeStruct((GC, SC), F32),
            jax.ShapeDtypeStruct((192, LC), F32),
            jax.ShapeDtypeStruct((GC, 128), F32),
        ),
        in_specs=[vmem] * 6,
        out_specs=[pl.BlockSpec(memory_space=pl.ANY)] * 4,
        scratch_shapes=[
            pltpu.VMEM((GC, 128), F32), pltpu.VMEM((192, LC), F32), pltpu.SemaphoreType.DMA((4,)),
        ],
        compiler_params=pltpu.CompilerParams(vmem_limit_bytes=24 * 1024 * 1024),
        name="finish",
    )(*[pltpu.with_memory_space_constraint(r, pltpu.VMEM) for r in results])


def on_device(gradient, left_factor, right_factor, left_basis, right_basis):
    return finish(*refresh(gradient, left_basis, right_basis, right_factor, left_factor))


def solution(mesh):
    in_specs = (P("row", "col"), P("row", "col"), P("col", "row"), P("row", "col"), P("row", "col"))
    out_specs = (P("row", "col"), P("col", "row"), P("row", "col"), P("col", "row"))
    return jax.shard_map(on_device, mesh=mesh, in_specs=in_specs, out_specs=out_specs, check_vma=False)
```

```python
import functools

import jax
import jax.numpy as jnp
from jax import lax
from jax.experimental import pallas as pl
from jax.experimental.pallas import tpu as pltpu
from jax.sharding import PartitionSpec as P

DMODEL = 3072
DHIDDEN = 14336
ema_decay = 0.95
epsilon = 1e-06
MESH = pl.DeviceIdType.MESH
F32 = jnp.float32
BF16 = jnp.bfloat16
GC = 1792
LC = 384
SC = 896
FIRST, SECOND = "f", "s"
TILES = ((0, 512), (512, 512), (1024, 512), (1536, 256))
PIECE = [n // 4 for _, n in TILES]
PLACE = [sum(PIECE[:t]) for t in range(len(TILES))]
A1, B1, C1, A2, B2, C2 = range(6)


def wrap(v):
    return (v + 1) % 4 - 1


def message_table():
    keys = []
    for h in (0, 1):
        for axis in (FIRST, SECOND):
            for d in (1, -1):
                keys.append((h, 0, 0, "full", axis, d))
        keys.append((h, -1, 0, 0, FIRST, 1))
        keys.append((h, 1, 0, 1, FIRST, -1))
        for df in (-1, 1, 2):
            for d in (1, -1):
                keys.append((h, df, 0, "full", SECOND, d))
        for df in (0, -1, 1, 2):
            keys.append((h, df, -1, 0, SECOND, 1))
            keys.append((h, df, 1, 1, SECOND, -1))
    return {key: i for i, key in enumerate(keys)}


AG = message_table()
UNITS = [
    (0, 0), (-1, 0), (1, 0), (0, -1), (0, 1), (2, 0), (-1, -1), (-1, 1), (1, -1), (1, 1),
    (0, 2), (2, -1), (2, 1), (-1, 2), (1, 2), (2, 2),
]
LAGS = (1, 2, 4)


def kernel(
    grad, lbas, rbas, rfac, lfac,
    acc, rout, rsum, ln, lpr, lsum,
    slab, lbuf, shared, bas, lp, away, near, both, whole,
    ra, tb, rb, rc, s1, keep, ra2, tb2, rb2, rc2, rsq,
    lsib, lmid, lrecv, lrows, lf, lsq,
    ag_s, ag_r, lg_s, lg_r, y_s, y_r, sib_s, sib_r, loc, bs, br, bss, bsr, cp,
    rs_s, rs_r, l0s, l0r, l1s, l1r, l2s, l2r, l4s, l4r, l3s, l3r, q_s, q_r,
):
    row = lax.axis_index("row")
    col = lax.axis_index("col")
    x, z = row // 4, row % 4
    y, k = col // 2, col % 2
    sib = {"col": y * 2 + (1 - k)}

    def ydev(d):
        return {"col": ((y + d + 4) % 4) * 2 + k}

    def rid(dx, dz):
        return ((x + dx + 4) % 4) * 4 + (z + dz + 4) % 4

    def region(ref, h, df, ds, part):
        dx, dz = (df, ds) if h == 0 else (ds, df)
        q, n = (0, 2) if part == "full" else (part, 1)
        return ref.at[pl.ds(rid(dx, dz) * 4 + 2 * h + q, n)]

    def neighbour(h, axis, d):
        if (h == 0) == (axis == FIRST):
            return {"row": ((x + d + 4) % 4) * 4 + z}
        return {"row": x * 4 + (z + d + 4) % 4}

    def ag(buf, ss, rr, h, df, ds, part, axis, d, arriving=False):
        if not arriving:
            key = (h, df, ds, part, axis, d)
        elif axis == FIRST:
            key = (h, wrap(df + d), ds, part, axis, d)
        else:
            key = (h, df, wrap(ds + d), part, axis, d)
        i = AG[key]
        ref = region(buf, h, df, ds, part)
        return pltpu.make_async_remote_copy(
            src_ref=ref, dst_ref=ref, send_sem=ss.at[i], recv_sem=rr.at[i],
            device_id=neighbour(h, axis, d), device_id_type=MESH,
        )

    def arrive(net, u):
        df, ds = UNITS[u]
        if u == 0:
            return
        axis = FIRST if ds == 0 else SECOND
        e = df if ds == 0 else ds
        for h in (0, 1):
            if e == 2:
                ag(*net, h, df, ds, 0, axis, 1, True).wait_recv()
                ag(*net, h, df, ds, 1, axis, -1, True).wait_recv()
            else:
                ag(*net, h, df, ds, "full", axis, -e, True).wait_recv()

    def onward(net, u):
        df, ds = UNITS[u]
        out = []
        if u == 0:
            for axis in (FIRST, SECOND):
                for h in (0, 1):
                    for d in (1, -1):
                        out.append((h, 0, 0, "full", axis, d))
        elif ds == 0:
            for h in (0, 1):
                if df == -1:
                    out.append((h, df, 0, 0, FIRST, 1))
                if df == 1:
                    out.append((h, df, 0, 1, FIRST, -1))
            for h in (0, 1):
                for d in (1, -1):
                    out.append((h, df, 0, "full", SECOND, d))
        elif ds != 2:
            for h in (0, 1):
                out.append((h, df, ds, 0 if ds == -1 else 1, SECOND, -ds))
        for key in out:
            c = ag(*net, *key)
            c.start()
            sent.append(c)

    sent = []
    G = (slab, ag_s, ag_r)
    L = (lbuf, lg_s, lg_r)

    own = [
        pltpu.make_async_copy(grad, slab.at[pl.ds(row * 4, 4)], cp.at[0]),
        pltpu.make_async_copy(lbas, lbuf.at[pl.ds(row * 4, 4)], cp.at[1]),
        pltpu.make_async_copy(rbas, bas.at[col], cp.at[2]),
    ]
    late = [
        pltpu.make_async_copy(rfac, acc, cp.at[3]),
        pltpu.make_async_copy(lfac, lf, cp.at[4]),
    ]
    for c in own + late:
        c.start()

    def colmate(i):
        return {"col": (col + i) % 8}

    def rowmate(i):
        return {"row": (row + i) % 16}

    barrier = pltpu.get_barrier_semaphore()

    def greet(make, n):
        def body(i, carry):
            pl.semaphore_signal(barrier, inc=1, device_id=make(i), device_id_type=MESH)
            return carry

        lax.fori_loop(1, n, body, 0)

    greet(colmate, 8)
    greet(rowmate, 16)
    for c in own:
        c.wait()
    pl.semaphore_wait(barrier, 22)

    is_k = k == z // 2
    role = (y - x + 4) % 4
    source = jnp.logical_and(is_k, role == 0)
    relay = jnp.logical_and(is_k, role != 0)
    c0 = pl.multiple_of((z % 2) * SC, 128)

    def unit_id(h, df, ds):
        return h * 16 + (df + 1) * 4 + ds + 1

    def unit_region(h, df, ds):
        return region(shared, h, df, ds, "full")

    def unit_src(h, df, ds):
        dx, dz = (df, ds) if h == 0 else (ds, df)
        return slab.at[pl.ds(rid(dx, dz) * 4 + 2 * h, 2), :, pl.ds(c0, SC)]

    def to_y(src, h, df, ds):
        i = unit_id(h, df, ds)
        return pltpu.make_async_remote_copy(
            src_ref=src, dst_ref=unit_region(h, df, ds), send_sem=y_s.at[i], recv_sem=y_r.at[i],
            device_id=ydev(1 if h == 0 else -1), device_id_type=MESH,
        )

    def to_sib(src, h, df, ds):
        i = unit_id(h, df, ds)
        return pltpu.make_async_remote_copy(
            src_ref=src, dst_ref=unit_region(h, df, ds), send_sem=sib_s.at[i], recv_sem=sib_r.at[i],
            device_id=sib, device_id_type=MESH,
        )

    def local(h, df, ds):
        return pltpu.make_async_copy(unit_src(h, df, ds), unit_region(h, df, ds), loc.at[unit_id(h, df, ds)])

    def last_role(h):
        return 3 if h == 0 else 1

    def source_unit(u):
        @pl.when(source)
        def _():
            df, ds = UNITS[u]
            for h in (0, 1):
                src = unit_src(h, df, ds)
                to_y(src, h, df, ds).start()
                to_sib(src, h, df, ds).start()
                local(h, df, ds).start()

    def hop(h):
        return role if h == 0 else (4 - role) % 4

    def relay_unit(hops, u):
        df, ds = UNITS[u]
        for h in (0, 1):

            @pl.when(jnp.logical_and(is_k, hop(h) == hops))
            def _():
                ref = unit_region(h, df, ds)
                to_y(ref, h, df, ds).wait_recv()
                if hops < 3:
                    to_y(ref, h, df, ds).start()
                to_sib(ref, h, df, ds).start()

    relayed = [0, 0, 0]

    def relay_to(hops, n):
        while relayed[hops - 1] < n:
            relay_unit(hops, relayed[hops - 1])
            relayed[hops - 1] += 1

    def b_ref(dy, kk, part):
        c = ((y + dy + 4) % 4) * 2 + kk
        return bas.at[c] if part == "full" else bas.at[c, part]

    def b_send(i, dy, part, d):
        ref = b_ref(dy, k, part)
        return pltpu.make_async_remote_copy(
            src_ref=ref, dst_ref=ref, send_sem=bs.at[i], recv_sem=br.at[i], device_id=ydev(d), device_id_type=MESH,
        )

    def b_sib(i, dy, kk):
        ref = b_ref(dy, kk, "full")
        return pltpu.make_async_remote_copy(
            src_ref=ref, dst_ref=ref, send_sem=bss.at[i], recv_sem=bsr.at[i], device_id=sib, device_id_type=MESH,
        )

    def group_ready(dx):
        units = [(0, dx, dz) for dz in (-1, 0, 1, 2)] + [(1, dz, dx) for dz in (-1, 0, 1, 2)]

        @pl.when(jnp.logical_not(is_k))
        def _():
            for u in units:
                to_sib(unit_region(*u), *u).wait_recv()

        @pl.when(source)
        def _():
            for u in units:
                local(*u).wait()

    def gram(dx, first, lo, hi):
        xg = (x + dx + 4) % 4
        rows = pl.ds(xg * 16, 16)

        for t in range(lo, hi):
            start, n = TILES[t]
            cols = pl.ds(start, n)
            a = slab[rows, :, cols].reshape(768, n)
            b = shared[rows].reshape(768, SC)
            d = lax.dot_general(a, b, (((0,), (0,)), ((), ())), preferred_element_type=F32)
            old = acc[cols, :]
            if first:
                old = ema_decay * old
            acc[cols, :] = old + (1.0 - ema_decay) * d

    def l0(yy, c):
        return pltpu.make_async_remote_copy(
            src_ref=lp.at[c], dst_ref=lsib.at[yy], send_sem=l0s.at[yy], recv_sem=l0r.at[yy],
            device_id=sib, device_id_type=MESH,
        )

    def left(dx):
        xg = (x + dx + 4) % 4

        def part(j, carry):
            c = xg * 2 + j
            a = slab[pl.ds(row * 4, 4)].reshape(192, GC)
            b = slab[pl.ds(xg * 16 + j * 8, 8)].reshape(384, GC)
            d = lax.dot_general(a, b, (((1,), (1,)), ((), ())), preferred_element_type=F32)
            lp[c] = d.astype(BF16)

            @pl.when(j != k)
            def _():
                l0(xg, c).start()

            return carry

        lax.fori_loop(0, 2, part, 0)

    def l1(dy):
        yy = (y + dy) % 4
        return pltpu.make_async_remote_copy(
            src_ref=lmid.at[yy], dst_ref=lrecv.at[y], send_sem=l1s.at[dy], recv_sem=l1r.at[dy],
            device_id={"col": yy * 2 + k}, device_id_type=MESH,
        )

    def l2(dy):
        return pltpu.make_async_remote_copy(
            src_ref=lrows.at[col], dst_ref=lrows.at[col], send_sem=l2s.at[dy], recv_sem=l2r.at[dy],
            device_id={"col": ((y + dy) % 4) * 2 + k}, device_id_type=MESH,
        )

    def l4(yy, kk):
        c = yy * 2 + kk
        return pltpu.make_async_remote_copy(
            src_ref=lrows.at[c], dst_ref=lrows.at[c], send_sem=l4s.at[yy], recv_sem=l4r.at[yy],
            device_id=sib, device_id_type=MESH,
        )

    def l3(i):
        return pltpu.make_async_remote_copy(
            src_ref=lsq.at[row], dst_ref=lsq.at[row], send_sem=l3s.at[i], recv_sem=l3r.at[i],
            device_id=rowmate(i), device_id_type=MESH,
        )

    def rq(i):
        return pltpu.make_async_remote_copy(
            src_ref=rsq.at[col], dst_ref=rsq.at[col], send_sem=q_s.at[i], recv_sem=q_r.at[i],
            device_id=colmate(i), device_id_type=MESH,
        )

    def each(n, make, what):
        def body(i, carry):
            c = make(i)
            getattr(c, what)()
            return carry

        lax.fori_loop(1, n, body, 0)

    def left_join():
        for dy in (1, 3, 2):
            yy = (y + dy) % 4
            l0(yy, yy * 2 + k).wait_recv()
            lmid[yy] = (lp[yy * 2 + k].astype(F32) + lsib[yy].astype(F32)).astype(BF16)
            l1(dy).start()

    def left_refresh():
        l0(y, col).wait_recv()
        total = lp[col].astype(F32) + lsib[y].astype(F32)
        for dy in (1, 3, 2):
            l1(dy).wait_recv()
            total = total + lrecv[(y + 4 - dy) % 4].astype(F32)
        new = ema_decay * lf[...] + (1.0 - ema_decay) * total
        ln[...] = new
        lrows[col] = new.astype(BF16)
        for dy in (1, 3, 2):
            l2(dy).start()
        l4(y, k).start()

    def left_share():
        for dy in (1, 3, 2):
            l2(dy).wait_recv()
            l4((y + 4 - dy) % 4, k).start()

    def left_product():
        for yy in range(4):
            l4(yy, 1 - k).wait_recv()

        def part(c, carry):
            b = lbuf[pl.ds(c * 8, 8)].reshape(384, LC)
            return carry + jnp.dot(lrows[c], b, preferred_element_type=F32)

        lpr[...] = lax.fori_loop(0, 8, part, jnp.zeros((192, LC), F32))
        v = lpr[...]
        lsq[row] = jnp.broadcast_to(jnp.sum(v * v, axis=0, keepdims=True), (8, LC))
        each(16, l3, "start")

    def make_product(t):
        lo, n = TILES[t]

        m = PIECE[t]

        def block(cc, carry):
            half = acc[pl.ds(lo, n), :].astype(BF16)
            for e in range(4):
                xo = (x + e) % 4
                d = jnp.dot(half, bas[xo * 2 + cc].reshape(SC, 256), preferred_element_type=F32)
                for i in range(4):
                    for s in (0, 1):
                        v = d[i * m : (i + 1) * m, s * 128 : (s + 1) * 128]
                        if i >= 2:
                            both[i - 2, cc * 2 + s, xo, spot(t), :] = v.astype(BF16)
                            whole[i - 2, cc * 2 + s, xo, spot(t), :] = v
                        elif e == 2:
                            away[i, 0, cc * 2 + s, spot(t), :] = v.astype(BF16)
                        elif e == (3 if i == 0 else 1):
                            away[i, 1, cc * 2 + s, spot(t), :] = v.astype(BF16)
                        else:
                            near[i, 0 if e == 0 else 1, cc * 2 + s, spot(t), :] = v
            return carry

        lax.fori_loop(0, 2, block, 0)

    TYPES = (0, 1, 2, 3)

    def hd(i):
        return i // 2, 1 if i % 2 == 0 else -1

    def rows_of(i, t):
        return pl.ds(TILES[t][0] + i * PIECE[t], PIECE[t])

    def spot(t):
        return pl.ds(PLACE[t], PIECE[t])

    def pos(h, axis):
        return x if (h == 0) == (axis == FIRST) else z

    def parcel(i, t, kind):
        h, d = hd(i)
        if h == 0:
            return away.at[i, 0 if kind == A1 else 1, :, spot(t), :]
        return both.at[i - 2, (z + (2 if kind == A1 else -d) + 4) % 4, :, spot(t), :]

    def kept(i, t, ahead):
        h, d = hd(i)
        if h == 0:
            return near.at[i, 1 if ahead else 0, :, spot(t), :]
        return whole.at[i - 2, (z + (d if ahead else 0) + 4) % 4, :, spot(t), :]

    def rs(kind, i, t):
        h, d = hd(i)
        axis = FIRST if kind < A2 else SECOND
        q = (pos(h, SECOND) + 4) % 4
        if kind == A1:
            src, dst, to = parcel(i, t, A1), ra.at[i, :, spot(t), :], d
        elif kind == B1:
            src, dst, to = tb.at[i, :, spot(t), :], rb.at[i, :, spot(t), :], d
        elif kind == C1:
            src, dst, to = parcel(i, t, C1), rc.at[i, :, spot(t), :], -d
        elif kind == A2:
            src, dst, to = s1.at[i, (q + 2) % 4, spot(t), :], ra2.at[i, spot(t), :], d
        elif kind == B2:
            src, dst, to = tb2.at[i, spot(t), :], rb2.at[i, spot(t), :], d
        else:
            src, dst, to = s1.at[i, (q - d + 4) % 4, spot(t), :], rc2.at[i, spot(t), :], -d
        return pltpu.make_async_remote_copy(
            src_ref=src, dst_ref=dst, send_sem=rs_s.at[kind, i * 4 + t], recv_sem=rs_r.at[kind, i * 4 + t],
            device_id=neighbour(h, axis, to), device_id_type=MESH,
        )

    def r0(t):
        for kind in (A1, C1):
            for i in TYPES:
                rs(kind, i, t).start()

    def r1(t):
        for i in TYPES:
            h, d = hd(i)
            rs(A1, i, t).wait_recv()
            tb[i, :, spot(t), :] = (kept(i, t, True)[...] + ra[i, :, spot(t), :].astype(F32)).astype(BF16)
            rs(B1, i, t).start()

    def r2(t):
        for i in TYPES:
            h, d = hd(i)
            rs(C1, i, t).wait_recv()
            rs(B1, i, t).wait_recv()
            total = kept(i, t, False)[...] + rb[i, :, spot(t), :].astype(F32) + rc[i, :, spot(t), :].astype(F32)
            s1[i, :, spot(t), :] = total.astype(BF16)
            rs(A2, i, t).start()
            rs(C2, i, t).start()
            q = pos(h, SECOND)
            for f, e in ((0, 0), (1, d)):
                w = (q + e + 4) % 4
                mine = kept(i, t, False).at[w]
                keep[f, i, spot(t), :] = (
                    mine[...] + rb[i, w, spot(t), :].astype(F32) + rc[i, w, spot(t), :].astype(F32)
                )

    def r3(t):
        for i in TYPES:
            h, d = hd(i)
            rs(A2, i, t).wait_recv()
            tb2[i, spot(t), :] = (keep[1, i, spot(t), :] + ra2[i, spot(t), :].astype(F32)).astype(BF16)
            rs(B2, i, t).start()

    def r4(t):
        total = jnp.zeros((8, 128), F32)
        for i in TYPES:
            rs(C2, i, t).wait_recv()
            rs(B2, i, t).wait_recv()
            v = keep[0, i, spot(t), :] + rb2[i, spot(t), :].astype(F32) + rc2[i, spot(t), :].astype(F32)
            rout[rows_of(i, t), :] = v
            total = total + jnp.sum((v * v).reshape(PIECE[t] // 8, 8, 128), axis=0)
        return total

    H = (0, 1)
    b_sends, b_sibs = [], []

    def begin(send, sibs):
        for c in send + sibs:
            c.start()
        b_sends.extend(send)
        b_sibs.extend(sibs)

    def lb(a, b):
        for u in range(a, b):
            arrive(L, u)
            onward(L, u)

    for u in range(16):
        arrive(G, u)
        onward(G, u)
        source_unit(u)
        for hops in (1, 2, 3):
            relay_to(hops, u + 1 - LAGS[hops - 1])
        if u == 2:
            begin([b_send(0, 0, "full", 1), b_send(1, 0, "full", -1)], [b_sib(0, 0, k)])
        if u == 8:
            b_send(0, -1, "full", 1).wait_recv()
            b_send(1, 1, "full", -1).wait_recv()
            begin([b_send(2, -1, 0, 1), b_send(3, 1, 1, -1)], [b_sib(1, -1, k), b_sib(2, 1, k)])
        if u == 12:
            onward(L, 0)
        if u == 15:
            lb(1, 3)
    relay_to(1, 16)
    lb(3, 6)
    relay_to(2, 16)
    late[0].wait()
    relay_to(3, 11)
    group_ready(0)
    gram(0, True, 0, 4)
    b_send(2, 2, 0, 1).wait_recv()
    b_send(3, 2, 1, -1).wait_recv()
    begin([], [b_sib(3, 2, k)])

    relay_to(3, 14)
    group_ready(-1)
    gram(-1, False, 0, 4)
    lb(6, 10)
    relay_to(3, 15)
    group_ready(1)
    gram(1, False, 0, 4)
    relay_to(3, 16)
    for i, dy in enumerate((0, -1, 1, 2)):
        b_sib(i, dy, 1 - k).wait_recv()
    group_ready(2)
    gram(2, False, 0, 1)
    make_product(0)
    r0(0)
    lb(10, 13)
    gram(2, False, 1, 2)
    make_product(1)
    r0(1)
    for dx in (0, -1, 1, 2):
        left(dx)
    r1(0)
    gram(2, False, 2, 3)
    make_product(2)
    r0(2)
    left_join()
    r1(1)
    gram(2, False, 3, 4)
    make_product(3)
    r0(3)
    r1(2)
    r2(0)
    late[1].wait()
    left_refresh()
    r1(3)
    r3(0)
    r2(1)
    total = r4(0)
    left_share()
    r3(1)
    r2(2)
    total = total + r4(1)
    lb(13, 16)
    left_product()
    r3(2)
    r2(3)
    total = total + r4(2)
    r3(3)
    total = total + r4(3)
    rsq[col] = total
    each(8, rq, "start")

    each(16, l3, "wait_recv")
    lsum[...] = jnp.sum(lsq[...], axis=0)
    each(8, rq, "wait_recv")
    rsum[...] = jnp.sum(rsq[...], axis=0)

    for c in sent + b_sends + b_sibs:
        c.wait_send()
    for df, ds in UNITS:
        for h in H:
            ref = unit_region(h, df, ds)

            @pl.when(jnp.logical_and(is_k, hop(h) != 3))
            def _():
                to_y(ref, h, df, ds).wait_send()

            @pl.when(is_k)
            def _():
                to_sib(ref, h, df, ds).wait_send()

    for kind in range(6):
        for i in TYPES:
            for t in range(4):
                rs(kind, i, t).wait_send()
    for yy in range(4):
        l0(yy, yy * 2 + 1 - k).wait_send()
        l4(yy, k).wait_send()
    for dy in (1, 2, 3):
        l1(dy).wait_send()
        l2(dy).wait_send()
    each(16, l3, "wait_send")
    each(8, rq, "wait_send")


def refresh(gradient, left_basis, right_basis, right_factor, left_factor):
    dma = pltpu.SemaphoreType.DMA
    n = len(AG)
    any_spec = pl.BlockSpec(memory_space=pl.ANY)
    V = pltpu.VMEM
    return pl.pallas_call(
        kernel,
        out_shape=(
            V((GC, SC), F32),
            V((GC, 128), F32),
            V((8, 128), F32),
            V((192, LC), F32),
            V((192, LC), F32),
            V((8, LC), F32),
        ),
        in_specs=[any_spec] * 5,
        out_specs=[pl.BlockSpec(memory_space=pltpu.VMEM)] * 6,
        scratch_shapes=[
            V((64, 48, GC), BF16), V((64, 48, LC), BF16), V((64, 48, SC), BF16),
            V((8, 2, 448, 256), BF16), V((8, 192, LC), BF16),
            V((2, 2, 4, 448, 128), BF16), V((2, 2, 4, 448, 128), F32),
            V((2, 4, 4, 448, 128), BF16), V((2, 4, 4, 448, 128), F32),
            V((4, 4, 448, 128), BF16), V((4, 4, 448, 128), BF16), V((4, 4, 448, 128), BF16),
            V((4, 4, 448, 128), BF16), V((4, 4, 448, 128), BF16), V((2, 4, 448, 128), F32),
            V((4, 448, 128), BF16), V((4, 448, 128), BF16), V((4, 448, 128), BF16), V((4, 448, 128), BF16),
            V((8, 8, 128), F32),
            V((4, 192, LC), BF16), V((4, 192, LC), BF16), V((4, 192, LC), BF16), V((8, 192, LC), BF16),
            V((192, LC), F32), V((16, 8, LC), F32),
            dma((n,)), dma((n,)), dma((n,)), dma((n,)),
            dma((32,)), dma((32,)), dma((32,)), dma((32,)), dma((32,)),
            dma((4,)), dma((4,)), dma((4,)), dma((4,)), dma((5,)),
            dma((6, 16)), dma((6, 16)),
            dma((4,)), dma((4,)), dma((4,)), dma((4,)), dma((4,)), dma((4,)), dma((4,)), dma((4,)),
            dma((16,)), dma((16,)), dma((8,)), dma((8,)),
        ],
        compiler_params=pltpu.CompilerParams(
            collective_id=0, has_side_effects=True, vmem_limit_bytes=58800000
        ),
        name="refresh",
    )(
        gradient.reshape(4, 48, GC), left_basis.reshape(4, 48, LC), right_basis.reshape(2, 448, 256),
        right_factor, left_factor,
    )


def finish_kernel(rnew, rprod, rsum, lnew, lprod, lsum, lnew_o, rnew_o, lout_o, rout_o, rout, lout, sem):
    copies = [pltpu.make_async_copy(rnew, rnew_o, sem.at[0]), pltpu.make_async_copy(lnew, lnew_o, sem.at[1])]
    for c in copies:
        c.start()
    right_sq = jnp.sum(rsum[...], axis=0, keepdims=True)
    rout[...] = rprod[...] * lax.rsqrt(right_sq / DHIDDEN + epsilon)
    copies.append(pltpu.make_async_copy(rout, rout_o, sem.at[2]))
    copies[2].start()
    lout[...] = lprod[...] * lax.rsqrt(lsum[:1, :] / DMODEL + epsilon)
    copies.append(pltpu.make_async_copy(lout, lout_o, sem.at[3]))
    copies[3].start()
    for c in copies:
        c.wait()


def finish(*results):
    vmem = pl.BlockSpec(memory_space=pltpu.VMEM)
    return pl.pallas_call(
        finish_kernel,
        out_shape=(
            jax.ShapeDtypeStruct((192, LC), F32),
            jax.ShapeDtypeStruct((GC, SC), F32),
            jax.ShapeDtypeStruct((192, LC), F32),
            jax.ShapeDtypeStruct((GC, 128), F32),
        ),
        in_specs=[vmem] * 6,
        out_specs=[pl.BlockSpec(memory_space=pl.ANY)] * 4,
        scratch_shapes=[
            pltpu.VMEM((GC, 128), F32), pltpu.VMEM((192, LC), F32), pltpu.SemaphoreType.DMA((4,)),
        ],
        compiler_params=pltpu.CompilerParams(vmem_limit_bytes=24 * 1024 * 1024),
        name="finish",
    )(*[pltpu.with_memory_space_constraint(r, pltpu.VMEM) for r in results])


def on_device(gradient, left_factor, right_factor, left_basis, right_basis):
    return finish(*refresh(gradient, left_basis, right_basis, right_factor, left_factor))


def solution(mesh):
    in_specs = (P("row", "col"), P("row", "col"), P("col", "row"), P("row", "col"), P("row", "col"))
    out_specs = (P("row", "col"), P("col", "row"), P("row", "col"), P("col", "row"))
    return jax.shard_map(on_device, mesh=mesh, in_specs=in_specs, out_specs=out_specs, check_vma=False)
```
